8 devices in a mesh: dp: 1 (over z), tp: 2 (over y), pp: 4 (over x, core).
Axes of the slice: x: 2, y: 2, z: 1, core: 2. Of those that a mesh axis runs over, the one named last changes fastest.
Arguments:
- x_micro: bfloat16 [8, 12, 512, 768], P(None, 'dp')
- ln1_gain: bfloat16 [4, 768], P('pp')
- ln1_bias: bfloat16 [4, 768], P('pp')
- w_qkv: bfloat16 [4, 3, 768, 12, 64], P('pp', None, None, 'tp')
- b_qkv: bfloat16 [4, 3, 12, 64], P('pp', None, 'tp')
- w_out: bfloat16 [4, 12, 64, 768], P('pp', 'tp')
- b_out: bfloat16 [4, 768], P('pp')
- ln2_gain: bfloat16 [4, 768], P('pp')
- ln2_bias: bfloat16 [4, 768], P('pp')
- w_up: bfloat16 [4, 768, 3072], P('pp', None, 'tp')
- b_up: bfloat16 [4, 3072], P('pp', 'tp')
- w_down: bfloat16 [4, 3072, 768], P('pp', 'tp')
- b_down: bfloat16 [4, 768], P('pp')
Outputs:
- output: bfloat16 [4, 8, 12, 512, 768], P('pp', None, 'dp')
All inputs are finite; a program needn't handle non-finite values.
Results may differ from the reference program's by a relative error of at most 0.0177418.
Values are sent between devices in bfloat16 or wider.
A program may use at most 1 GiB of HBM per device.

```python
import jax
import jax.numpy as jnp
from jax import lax

LAYERS = 4
MICRO_BATCHES = 8
MB_ROWS = 12
SEQ_LEN = 512
D_MODEL = 768
N_HEADS = 12
HEAD_DIM = 64
FF_DIM = 3072
LN_EPS = 1e-5


def setup_inputs(seed: int = 0, part: int = 0) -> dict:
    base_key = jax.random.key(seed)
    key_list = jax.random.split(base_key, 13)
    x_key = jax.random.fold_in(key_list[0], part)

    def normal_bf16(key_in, shape_dims, scale_by, centre=0.0):
        sample_f32 = jax.random.normal(key_in, shape_dims, jnp.float32) * scale_by + centre
        return sample_f32.astype(jnp.bfloat16)

    return {
        'x_micro': normal_bf16(x_key, (MICRO_BATCHES, MB_ROWS, SEQ_LEN, D_MODEL), 1.0),
        'ln1_gain': normal_bf16(key_list[1], (LAYERS, D_MODEL), 0.2, 1.0),
        'ln1_bias': normal_bf16(key_list[2], (LAYERS, D_MODEL), 0.2),
        'w_qkv': normal_bf16(key_list[3], (LAYERS, 3, D_MODEL, N_HEADS, HEAD_DIM), D_MODEL ** -0.5),
        'b_qkv': normal_bf16(key_list[4], (LAYERS, 3, N_HEADS, HEAD_DIM), 0.5),
        'w_out': normal_bf16(key_list[5], (LAYERS, N_HEADS, HEAD_DIM, D_MODEL), (N_HEADS * HEAD_DIM) ** -0.5),
        'b_out': normal_bf16(key_list[6], (LAYERS, D_MODEL), 0.2),
        'ln2_gain': normal_bf16(key_list[7], (LAYERS, D_MODEL), 0.2, 1.0),
        'ln2_bias': normal_bf16(key_list[8], (LAYERS, D_MODEL), 0.2),
        'w_up': normal_bf16(key_list[9], (LAYERS, D_MODEL, FF_DIM), D_MODEL ** -0.5),
        'b_up': normal_bf16(key_list[10], (LAYERS, FF_DIM), 0.2),
        'w_down': normal_bf16(key_list[11], (LAYERS, FF_DIM, D_MODEL), FF_DIM ** -0.5),
        'b_down': normal_bf16(key_list[12], (LAYERS, D_MODEL), 0.2),
    }


def layer_norm(act_in, gain_vec, bias_vec):
    act_f32 = act_in.astype(jnp.float32)
    row_mean = jnp.mean(act_f32, axis=-1, keepdims=True)
    centered = act_f32 - row_mean
    row_var = jnp.mean(centered * centered, axis=-1, keepdims=True)
    normed = centered * lax.rsqrt(row_var + LN_EPS)
    return (normed * gain_vec.astype(jnp.float32) + bias_vec.astype(jnp.float32)).astype(jnp.bfloat16)


def one_layer(act_in, layer_params):
    ln1_gain, ln1_bias, w_qkv, b_qkv, w_out, b_out, ln2_gain, ln2_bias, w_up, b_up, w_down, b_down = layer_params
    token_rows = MB_ROWS * SEQ_LEN
    head_width = N_HEADS * HEAD_DIM
    flat_in = act_in.reshape(token_rows, D_MODEL)
    normed_in = layer_norm(flat_in, ln1_gain, ln1_bias)
    w_flat = w_qkv.reshape(3, D_MODEL, head_width)
    b_flat = b_qkv.reshape(3, head_width).astype(jnp.float32)
    projected = [
        (jnp.dot(normed_in, w_flat[proj_idx], preferred_element_type=jnp.float32) + b_flat[proj_idx])
        .astype(jnp.bfloat16).astype(jnp.float32).reshape(MB_ROWS, SEQ_LEN, N_HEADS, HEAD_DIM)
        for proj_idx in range(3)
    ]
    query_f, key_f, value_f = projected
    scores = jnp.einsum('bqhd,bkhd->bhqk', query_f, key_f) * (HEAD_DIM ** -0.5)
    causal = lax.broadcasted_iota(jnp.int32, (SEQ_LEN, SEQ_LEN), 0) >= lax.broadcasted_iota(jnp.int32, (SEQ_LEN, SEQ_LEN), 1)
    scores = jnp.where(causal, scores, -1e30)
    attn_probs = jax.nn.softmax(scores, axis=-1).astype(jnp.bfloat16).astype(jnp.float32)
    context = jnp.einsum('bhqk,bkhd->bqhd', attn_probs, value_f).astype(jnp.bfloat16)
    attn_out = (jnp.dot(context.reshape(token_rows, head_width), w_out.reshape(head_width, D_MODEL), preferred_element_type=jnp.float32) + b_out.astype(jnp.float32)).astype(jnp.bfloat16)
    resid_mid = (flat_in.astype(jnp.float32) + attn_out.astype(jnp.float32)).astype(jnp.bfloat16)
    normed_mid = layer_norm(resid_mid, ln2_gain, ln2_bias)
    hidden_up = jax.nn.gelu(jnp.dot(normed_mid, w_up, preferred_element_type=jnp.float32) + b_up.astype(jnp.float32), approximate=True).astype(jnp.bfloat16)
    mlp_out = (jnp.dot(hidden_up, w_down, preferred_element_type=jnp.float32) + b_down.astype(jnp.float32)).astype(jnp.bfloat16)
    result = (resid_mid.astype(jnp.float32) + mlp_out.astype(jnp.float32)).astype(jnp.bfloat16)
    return result.reshape(MB_ROWS, SEQ_LEN, D_MODEL)


def reference(x_micro, ln1_gain, ln1_bias, w_qkv, b_qkv, w_out, b_out, ln2_gain, ln2_bias, w_up, b_up, w_down, b_down):
    stacked_params = (ln1_gain, ln1_bias, w_qkv, b_qkv, w_out, b_out, ln2_gain, ln2_bias, w_up, b_up, w_down, b_down)

    def layer_step(micro_acts, layer_params):
        new_acts = lax.map(lambda micro_in: one_layer(micro_in, layer_params), micro_acts)
        return new_acts, new_acts

    final_acts, y_all = lax.scan(layer_step, x_micro, stacked_params)
    return y_all
```

```python
import functools
import math

import jax
import jax.numpy as jnp
from jax import lax
from jax.experimental import pallas as pl
from jax.experimental.pallas import tpu as pltpu
from jax.sharding import PartitionSpec as P

F32 = jnp.float32
BF16 = jnp.bfloat16
MESH = pl.DeviceIdType.MESH
LN_EPS = 1e-5
N_DUP = 0
IN_SLOTS = 3
OUT_SLOTS = 2
QUERY_BLOCK = 256
COL_BLOCK = 256
GELU_C0 = math.sqrt(2.0 / math.pi)
GELU_C1 = GELU_C0 * 0.044715


def dot(a, b, ca=1, cb=0):
    return lax.dot_general(a, b, (((ca,), (cb,)), ((), ())), preferred_element_type=F32)


def layer_norm(x, gain, bias):
    x = x.astype(F32)
    mean = jnp.mean(x, axis=-1, keepdims=True)
    centered = x - mean
    var = jnp.mean(centered * centered, axis=-1, keepdims=True)
    return (centered * lax.rsqrt(var + LN_EPS) * gain.astype(F32) + bias.astype(F32)).astype(BF16)


def gelu(z):
    half = 0.5 * z
    return half + half * jnp.tanh(z * (GELU_C0 + GELU_C1 * (z * z)))


def attention(qkv, ctx, head_dim):
    seq, width = ctx.shape
    pair = 2 * head_dim
    scale = head_dim**-0.5 * math.log2(math.e)
    first = lax.broadcasted_iota(jnp.int32, (1, pair), 1) < head_dim
    zero = jnp.zeros((), BF16)
    block = QUERY_BLOCK
    rows = lax.broadcasted_iota(jnp.int32, (block, block), 0)
    cols = lax.broadcasted_iota(jnp.int32, (block, block), 1)
    keep = jnp.concatenate([rows >= cols, rows >= cols], axis=0)
    for p in range(width // pair):
        lanes = slice(p * pair, (p + 1) * pair)
        keys = qkv[:, width + p * pair : width + (p + 1) * pair]
        values = qkv[:, 2 * width + p * pair : 2 * width + (p + 1) * pair]
        for q0 in range(0, seq, block):
            q = qkv[q0 : q0 + block, lanes]
            q = jnp.concatenate([jnp.where(first, q, zero), jnp.where(first, zero, q)], axis=0)
            scores = dot(q, keys[: q0 + block], 1, 1)
            diag = jnp.where(keep, scores[:, q0:], -1e30)
            scores = jnp.concatenate([scores[:, :q0], diag], axis=1) if q0 else diag
            top = jnp.max(scores, axis=-1, keepdims=True)
            probs = jnp.exp2((scores - top) * scale)
            total = jnp.sum(probs, axis=-1, keepdims=True)
            out = dot(probs.astype(BF16), values[: q0 + block]) * (1.0 / total)
            ctx[q0 : q0 + block, lanes] = jnp.where(first, out[:block], out[block:]).astype(BF16)


def project_residual(lhs, weight, bias, resid, out):
    for n in range(0, out.shape[1], COL_BLOCK):
        cols = slice(n, n + COL_BLOCK)
        part = (dot(lhs[...], weight[:, cols]) + bias[:, cols].astype(F32)).astype(BF16)
        out[:, cols] = (resid[:, cols].astype(F32) + part.astype(F32)).astype(BF16)


def one_layer(x, y, w, s, head_dim):
    width = x.shape[1]
    s["h"][...] = layer_norm(x[...], w["g1"][...], w["c1"][...])
    for n in range(0, 3 * width, COL_BLOCK):
        cols = slice(n, n + COL_BLOCK)
        s["qkv"][:, cols] = (dot(s["h"][...], w["qkv"][:, cols]) + w["bqkv"][:, cols]).astype(BF16)
    attention(s["qkv"], s["ctx"], head_dim)
    project_residual(s["ctx"], w["out"], w["bout"], x, s["x1"])
    s["h"][...] = layer_norm(s["x1"][...], w["g2"][...], w["c2"][...])
    half = w["up"].shape[2]
    for t in range(2):
        for n in range(0, half, COL_BLOCK):
            z = dot(s["h"][...], w["up"][t, :, n : n + COL_BLOCK]) + w["bup"][t, :, n : n + COL_BLOCK].astype(F32)
            s["u"][:, t * half + n : t * half + n + COL_BLOCK] = gelu(z).astype(BF16)
    project_residual(s["u"], w["down"], w["bdown"], s["x1"], y)


def kernel(
    cfg,
    x_hbm, g1, c1, bout, g2, c2, bdown, qkv_half, bqkv_half, out_half, up_half, bup_half, down_half,
    out_hbm,
    w_qkv, b_qkv_raw, b_qkv, w_out, w_up, b_up, w_down,
    x_in, y_out, h, qkv, ctx, x1, u,
    w_local, w_send, w_recv, in_sem, store_sem, hop_sem, side_send, side_recv, credit,
):
    stages, n_single, n_dup, head_dim = cfg
    total = n_single + n_dup
    t = lax.axis_index("tp")
    p = lax.axis_index("pp")
    width = x_hbm.shape[2]
    half_width = width // 2
    other = {"tp": 1 - t}
    after = {"pp": lax.rem(p + 1, stages)}
    before = {"pp": lax.rem(p + stages - 1, stages)}

    barrier = pltpu.get_barrier_semaphore()
    for peer in (other, after, before):
        pl.semaphore_signal(barrier, inc=1, device_id=peer, device_id_type=MESH)
    pl.semaphore_wait(barrier, 3)

    pieces = []
    for c in range(3):
        at = pl.multiple_of(c * width + t * half_width, 128)
        pieces.append((qkv_half.at[c], w_qkv.at[:, pl.ds(at, half_width)]))
    pieces.append((bqkv_half, b_qkv_raw.at[t]))
    pieces.append((out_half, w_out.at[pl.ds(pl.multiple_of(t * half_width, 128), half_width)]))
    pieces.append((up_half, w_up.at[t]))
    pieces.append((bup_half, b_up.at[t]))
    pieces.append((down_half, w_down.at[pl.ds(pl.multiple_of(t * down_half.shape[0], 128), down_half.shape[0])]))
    copies = []
    for i, (src, dst) in enumerate(pieces):
        far = pltpu.make_async_remote_copy(src, dst, w_send.at[i], w_recv.at[i], device_id=other, device_id_type=MESH)
        near = pltpu.make_async_copy(src, dst, w_local.at[i])
        far.start()
        near.start()
        copies.append((far, near))

    def row_of(n):
        dup = n // n_single
        return n + (1 - dup) * t * n_single + dup * n_single

    def load(n):
        slot = lax.rem(n, IN_SLOTS)
        return pltpu.make_async_copy(x_hbm.at[row_of(n)], x_in.at[slot], in_sem.at[slot])

    def store(n):
        slot = lax.rem(n, OUT_SLOTS)
        return pltpu.make_async_copy(y_out.at[slot], out_hbm.at[row_of(n)], store_sem.at[slot])

    def hop(n):
        src, dst = lax.rem(n, OUT_SLOTS), lax.rem(n, IN_SLOTS)
        return pltpu.make_async_remote_copy(
            y_out.at[src], x_in.at[dst], hop_sem.at[src], in_sem.at[dst], device_id=after, device_id_type=MESH
        )

    def side(n):
        row = row_of(n)
        return pltpu.make_async_remote_copy(
            out_hbm.at[row], out_hbm.at[row], side_send.at[n], side_recv.at[n], device_id=other, device_id_type=MESH
        )

    @pl.when(p == 0)
    def _():
        load(0).start()

    for far, near in copies:
        near.wait()
        far.wait_recv()
    for c in range(3):
        for k in range(2):
            at = c * width + k * half_width
            b_qkv[:, at : at + half_width] = b_qkv_raw[k, :, c * half_width : (c + 1) * half_width].astype(F32)

    weights = dict(
        g1=g1, c1=c1, qkv=w_qkv, bqkv=b_qkv, out=w_out, bout=bout, g2=g2, c2=c2,
        up=w_up, bup=b_up, down=w_down, bdown=bdown,
    )
    scratch = dict(h=h, qkv=qkv, ctx=ctx, x1=x1, u=u)

    def step(n, carry):
        in_slot, out_slot = lax.rem(n, IN_SLOTS), lax.rem(n, OUT_SLOTS)
        load(n).wait()

        @pl.when((p == 0) & (n + 1 < total))
        def _():
            load(n + 1).start()

        @pl.when(n >= OUT_SLOTS)
        def _():
            @pl.when(p < stages - 1)
            def _():
                hop(n - OUT_SLOTS).wait_send()

        one_layer(x_in.at[in_slot], y_out.at[out_slot], weights, scratch, head_dim)

        @pl.when((p > 0) & (n + IN_SLOTS < total))
        def _():
            pl.semaphore_signal(credit, inc=1, device_id=before, device_id_type=MESH)

        @pl.when(p < stages - 1)
        def _():
            @pl.when(n >= IN_SLOTS)
            def _():
                pl.semaphore_wait(credit, 1)

            hop(n).start()

        put = store(n)
        put.start()
        put.wait()

        @pl.when(n < n_single)
        def _():
            side(n).start()

        return carry

    lax.fori_loop(0, total, step, 0)

    @pl.when(p < stages - 1)
    def _():
        for n in range(total - OUT_SLOTS, total):
            hop(n).wait_send()

    for far, near in copies:
        far.wait_send()

    def finish(n, carry):
        side(n).wait_send()
        side(n).wait_recv()
        return carry

    lax.fori_loop(0, n_single, finish, 0)


def solution(mesh):
    stages = mesh.shape["pp"]
    weight_specs = (
        P("pp", None), P("pp", None),
        P("pp", None, None, "tp", None), P("pp", None, "tp", None),
        P("pp", "tp", None, None), P("pp", None),
        P("pp", None), P("pp", None),
        P("pp", None, "tp"), P("pp", "tp"),
        P("pp", "tp", None), P("pp", None),
    )

    def local_run(x_micro, g1, c1, w_qkv, b_qkv, w_out, b_out, g2, c2, w_up, b_up, w_down, b_down):
        micro, rows, seq, width = x_micro.shape
        count = micro * rows
        heads, head_dim = w_qkv.shape[3:]
        half_width = heads * head_dim
        half_ff = w_up.shape[2]
        n_dup = N_DUP
        n_single = (count - n_dup) // 2
        cfg = (stages, n_single, n_dup, head_dim)
        operands = (
            x_micro.reshape(count, seq, width),
            g1, c1, b_out, g2, c2, b_down,
            w_qkv.reshape(3, width, half_width),
            b_qkv.reshape(1, 3 * half_width),
            w_out.reshape(half_width, width),
            w_up.reshape(width, half_ff),
            b_up.reshape(1, half_ff),
            w_down.reshape(half_ff, width),
        )
        anywhere = pl.BlockSpec(memory_space=pl.ANY)
        vmem = pl.BlockSpec(memory_space=pltpu.VMEM)
        out = pl.pallas_call(
            functools.partial(kernel, cfg),
            out_shape=jax.ShapeDtypeStruct((count, seq, width), BF16),
            in_specs=[anywhere] + [vmem] * 6 + [anywhere] * 6,
            out_specs=anywhere,
            scratch_shapes=[
                pltpu.VMEM((width, 3 * width), BF16),
                pltpu.VMEM((2, 1, 3 * half_width), BF16),
                pltpu.VMEM((1, 3 * width), F32),
                pltpu.VMEM((width, width), BF16),
                pltpu.VMEM((2, width, half_ff), BF16),
                pltpu.VMEM((2, 1, half_ff), BF16),
                pltpu.VMEM((2 * half_ff, width), BF16),
                pltpu.VMEM((IN_SLOTS, seq, width), BF16),
                pltpu.VMEM((OUT_SLOTS, seq, width), BF16),
                pltpu.VMEM((seq, width), BF16),
                pltpu.VMEM((seq, 3 * width), BF16),
                pltpu.VMEM((seq, width), BF16),
                pltpu.VMEM((seq, width), BF16),
                pltpu.VMEM((seq, 2 * half_ff), BF16),
                pltpu.SemaphoreType.DMA((8,)),
                pltpu.SemaphoreType.DMA((8,)),
                pltpu.SemaphoreType.DMA((8,)),
                pltpu.SemaphoreType.DMA((IN_SLOTS,)),
                pltpu.SemaphoreType.DMA((OUT_SLOTS,)),
                pltpu.SemaphoreType.DMA((OUT_SLOTS,)),
                pltpu.SemaphoreType.DMA((n_single,)),
                pltpu.SemaphoreType.DMA((n_single,)),
                pltpu.SemaphoreType.REGULAR,
            ],
            compiler_params=pltpu.CompilerParams(
                collective_id=0, has_side_effects=True, vmem_limit_bytes=60 * 2**20
            ),
        )(*operands)
        return out.reshape(1, micro, rows, seq, width)

    return jax.shard_map(
        local_run,
        mesh=mesh,
        in_specs=(P(None, "dp", None, None),) + weight_specs,
        out_specs=P("pp", None, "dp", None, None),
        check_vma=False,
    )
```

```python
import functools
import math

import jax
import jax.numpy as jnp
from jax import lax
from jax.experimental import pallas as pl
from jax.experimental.pallas import tpu as pltpu
from jax.sharding import PartitionSpec as P

F32 = jnp.float32
BF16 = jnp.bfloat16
MESH = pl.DeviceIdType.MESH
LN_EPS = 1e-5
N_DUP = 16
IN_SLOTS = 3
OUT_SLOTS = 2
QUERY_BLOCK = 256
COL_BLOCK = 256
ROW_BLOCK = 128
GELU_C0 = math.sqrt(2.0 / math.pi)
GELU_C1 = GELU_C0 * 0.044715


def dot(a, b, ca=1, cb=0):
    return lax.dot_general(a, b, (((ca,), (cb,)), ((), ())), preferred_element_type=F32)


def layer_norm(x, gain, bias):
    x = x.astype(F32)
    mean = jnp.mean(x, axis=-1, keepdims=True)
    centered = x - mean
    var = jnp.mean(centered * centered, axis=-1, keepdims=True)
    return (centered * lax.rsqrt(var + LN_EPS) * gain.astype(F32) + bias.astype(F32)).astype(BF16)


def gelu(z):
    return z * jax.nn.sigmoid(z * (2.0 * GELU_C0 + 2.0 * GELU_C1 * (z * z)))


def attention(qkv, ctx, head_dim):
    seq, width = ctx.shape
    pair = 2 * head_dim
    scale = head_dim**-0.5 * math.log2(math.e)
    first = lax.broadcasted_iota(jnp.int32, (1, pair), 1) < head_dim
    zero = jnp.zeros((), BF16)
    block = QUERY_BLOCK
    keep = lax.broadcasted_iota(jnp.int32, (block, block), 0) >= lax.broadcasted_iota(jnp.int32, (block, block), 1)
    keep = jnp.concatenate([keep, keep], axis=0)
    for q0 in range(seq - block, -1, -block):
        for p in range(width // pair):
            lanes = slice(p * pair, (p + 1) * pair)
            keys = qkv[: q0 + block, width + p * pair : width + (p + 1) * pair]
            values = qkv[: q0 + block, 2 * width + p * pair : 2 * width + (p + 1) * pair]
            q = qkv[q0 : q0 + block, lanes]
            q = jnp.concatenate([jnp.where(first, q, zero), jnp.where(first, zero, q)], axis=0)
            scores = dot(q, keys, 1, 1)
            diag = jnp.where(keep, scores[:, q0:], -1e30)
            scores = jnp.concatenate([scores[:, :q0], diag], axis=1) if q0 else diag
            top = jnp.max(scores, axis=-1, keepdims=True)
            probs = jnp.exp2((scores - top) * scale)
            total = jnp.sum(probs, axis=-1, keepdims=True)
            out = dot(probs.astype(BF16), values) * (1.0 / total)
            ctx[q0 : q0 + block, lanes] = jnp.where(first, out[:block], out[block:]).astype(BF16)


def project_residual(lhs, weight, bias, resid, out, rows):
    for n in range(0, out.shape[1], COL_BLOCK):
        cols = slice(n, n + COL_BLOCK)
        part = (dot(lhs[rows], weight[:, cols]) + bias[:, cols].astype(F32)).astype(BF16)
        out[rows, cols] = (resid[rows, cols].astype(F32) + part.astype(F32)).astype(BF16)


def one_layer(x, y, w, s, head_dim, between):
    seq, width = x.shape
    blocks = [slice(m, m + ROW_BLOCK) for m in range(0, seq, ROW_BLOCK)]
    for rows in blocks:
        s["h"][rows] = layer_norm(x[rows], w["g1"][...], w["c1"][...])
        for n in range(0, 3 * width, COL_BLOCK):
            cols = slice(n, n + COL_BLOCK)
            s["qkv"][rows, cols] = (dot(s["h"][rows], w["qkv"][:, cols]) + w["bqkv"][:, cols]).astype(BF16)
    between()
    attention(s["qkv"], s["ctx"], head_dim)
    for rows in blocks:
        project_residual(s["ctx"], w["out"], w["bout"], x, s["x1"], rows)
        s["h"][rows] = layer_norm(s["x1"][rows], w["g2"][...], w["c2"][...])
    half = w["up"].shape[2]
    for t in range(2):
        for n in range(0, half, COL_BLOCK):
            for rows in blocks:
                z = dot(s["h"][rows], w["up"][t, :, n : n + COL_BLOCK])
                z = z + w["bup"][t, :, n : n + COL_BLOCK].astype(F32)
                s["u"][rows, t * half + n : t * half + n + COL_BLOCK] = gelu(z).astype(BF16)
    for n in range(0, width, COL_BLOCK):
        for rows in blocks:
            cols = slice(n, n + COL_BLOCK)
            part = (dot(s["u"][rows], w["down"][:, cols]) + w["bdown"][:, cols].astype(F32)).astype(BF16)
            y[rows, cols] = (s["x1"][rows, cols].astype(F32) + part.astype(F32)).astype(BF16)


def kernel(
    cfg,
    x_hbm, g1, c1, bout, g2, c2, bdown, qkv_half, bqkv_half, out_half, up_half, bup_half, down_half,
    out_hbm,
    w_qkv_raw, w_qkv, b_qkv_raw, b_qkv, w_out, w_up, b_up, w_down,
    x_in, y_out, h, qkv, ctx, x1, u,
    w_local, w_send, w_recv, in_sem, store_sem, hop_sem, side_send, side_recv, credit, turn,
):
    stages, n_single, n_dup, head_dim = cfg
    total = n_single + n_dup
    t = lax.axis_index("tp")
    p = lax.axis_index("pp")
    width = x_hbm.shape[2]
    half_width = width // 2
    other = {"tp": 1 - t}
    after = {"pp": lax.rem(p + 1, stages)}
    before = {"pp": lax.rem(p + stages - 1, stages)}

    barrier = pltpu.get_barrier_semaphore()
    for peer in (other, after, before):
        pl.semaphore_signal(barrier, inc=1, device_id=peer, device_id_type=MESH)
    pl.semaphore_wait(barrier, 3)

    half_ff = down_half.shape[0]
    mine = pl.ds(pl.multiple_of(t * half_width, 128), half_width)
    pieces = [(qkv_half.at[c], w_qkv_raw.at[c, mine]) for c in range(3)]
    pieces.append((bqkv_half, b_qkv_raw.at[t]))
    pieces.append((out_half, w_out.at[mine]))
    pieces.append((bup_half, b_up.at[t]))
    pieces.append((up_half, w_up.at[t]))
    pieces.append((down_half, w_down.at[pl.ds(pl.multiple_of(t * half_ff, 128), half_ff)]))
    near, far = [], []
    for i, (src, dst) in enumerate(pieces):
        near.append(pltpu.make_async_copy(src, dst, w_local.at[i]))
        far.append(
            pltpu.make_async_remote_copy(src, dst, w_send.at[i], w_recv.at[i], device_id=other, device_id_type=MESH)
        )
        near[-1].start()

    @pl.when(lax.rem(p, 2) == 1)
    def _():
        pl.semaphore_wait(turn, 1)

    for copy in far:
        copy.start()

    def row_of(n):
        dup = n // n_single
        return n + (1 - dup) * t * n_single + dup * n_single

    def load(n):
        slot = lax.rem(n, IN_SLOTS)
        return pltpu.make_async_copy(x_hbm.at[row_of(n)], x_in.at[slot], in_sem.at[slot])

    def store(n):
        slot = lax.rem(n, OUT_SLOTS)
        return pltpu.make_async_copy(y_out.at[slot], out_hbm.at[row_of(n)], store_sem.at[slot])

    def hop(n):
        src, dst = lax.rem(n, OUT_SLOTS), lax.rem(n, IN_SLOTS)
        return pltpu.make_async_remote_copy(
            y_out.at[src], x_in.at[dst], hop_sem.at[src], in_sem.at[dst], device_id=after, device_id_type=MESH
        )

    def side(n):
        row = row_of(n)
        return pltpu.make_async_remote_copy(
            out_hbm.at[row], out_hbm.at[row], side_send.at[n], side_recv.at[n], device_id=other, device_id_type=MESH
        )

    @pl.when(p == 0)
    def _():
        load(0).start()

    def arrived(i):
        near[i].wait()
        far[i].wait_recv()

    for i in range(4):
        arrived(i)
    for c in range(3):
        for m in range(0, width, COL_BLOCK):
            w_qkv[:, c * width + m : c * width + m + COL_BLOCK] = w_qkv_raw[c, m : m + COL_BLOCK, :].T
        for k in range(2):
            for head in range(half_width // head_dim):
                at = c * width + k * half_width + head * head_dim
                b_qkv[:, at : at + head_dim] = b_qkv_raw[k, c, head : head + 1, :].astype(F32)
    for copy in far:
        copy.wait_send()

    @pl.when(lax.rem(p, 2) == 0)
    def _():
        pl.semaphore_signal(turn, inc=1, device_id=after, device_id_type=MESH)

    for i in range(4, len(far)):
        arrived(i)

    weights = dict(
        g1=g1, c1=c1, qkv=w_qkv, bqkv=b_qkv, out=w_out, bout=bout, g2=g2, c2=c2,
        up=w_up, bup=b_up, down=w_down, bdown=bdown,
    )
    scratch = dict(h=h, qkv=qkv, ctx=ctx, x1=x1, u=u)

    def publish(n):
        store(n).wait()

        @pl.when(n < n_single)
        def _():
            side(n).start()

    def step(n, carry):
        in_slot, out_slot = lax.rem(n, IN_SLOTS), lax.rem(n, OUT_SLOTS)
        load(n).wait()

        @pl.when((p == 0) & (n + 1 < total))
        def _():
            load(n + 1).start()

        @pl.when((n >= OUT_SLOTS) & (p < stages - 1))
        def _():
            hop(n - OUT_SLOTS).wait_send()

        def between():
            @pl.when(n >= 1)
            def _():
                publish(n - 1)

        one_layer(x_in.at[in_slot], y_out.at[out_slot], weights, scratch, head_dim, between)

        store(n).start()

        @pl.when((p < stages - 1) & (n >= IN_SLOTS))
        def _():
            pl.semaphore_wait(credit, 1)

        @pl.when(p < stages - 1)
        def _():
            hop(n).start()

        @pl.when((p > 0) & (n + IN_SLOTS < total))
        def _():
            pl.semaphore_signal(credit, inc=1, device_id=before, device_id_type=MESH)

        return carry

    lax.fori_loop(0, total, step, 0)
    publish(total - 1)

    @pl.when(p < stages - 1)
    def _():
        for n in range(total - OUT_SLOTS, total):
            hop(n).wait_send()

    def finish(n, carry):
        side(n).wait_send()
        side(n).wait_recv()
        return carry

    lax.fori_loop(0, n_single, finish, 0)


def solution(mesh):
    stages = mesh.shape["pp"]
    weight_specs = (
        P("pp", None), P("pp", None),
        P("pp", None, None, "tp", None), P("pp", None, "tp", None),
        P("pp", "tp", None, None), P("pp", None),
        P("pp", None), P("pp", None),
        P("pp", None, "tp"), P("pp", "tp"),
        P("pp", "tp", None), P("pp", None),
    )

    def local_run(x_micro, g1, c1, w_qkv, b_qkv, w_out, b_out, g2, c2, w_up, b_up, w_down, b_down):
        micro, rows, seq, width = x_micro.shape
        count = micro * rows
        heads, head_dim = w_qkv.shape[3:]
        half_width = heads * head_dim
        half_ff = w_up.shape[2]
        n_dup = N_DUP
        n_single = (count - n_dup) // 2
        cfg = (stages, n_single, n_dup, head_dim)
        operands = (
            x_micro.reshape(count, seq, width),
            g1, c1, b_out, g2, c2, b_down,
            w_qkv.reshape(3, width, heads, head_dim).transpose(0, 2, 3, 1).reshape(3, half_width, width),
            b_qkv.reshape(3, heads, head_dim),
            w_out.reshape(half_width, width),
            w_up.reshape(width, half_ff),
            b_up.reshape(1, half_ff),
            w_down.reshape(half_ff, width),
        )
        anywhere = pl.BlockSpec(memory_space=pl.ANY)
        vmem = pl.BlockSpec(memory_space=pltpu.VMEM)
        out = pl.pallas_call(
            functools.partial(kernel, cfg),
            out_shape=jax.ShapeDtypeStruct((count, seq, width), BF16),
            in_specs=[anywhere] + [vmem] * 6 + [anywhere] * 6,
            out_specs=anywhere,
            scratch_shapes=[
                pltpu.VMEM((3, width, width), BF16),
                pltpu.VMEM((width, 3 * width), BF16),
                pltpu.VMEM((2, 3, heads, head_dim), BF16),
                pltpu.VMEM((1, 3 * width), F32),
                pltpu.VMEM((width, width), BF16),
                pltpu.VMEM((2, width, half_ff), BF16),
                pltpu.VMEM((2, 1, half_ff), BF16),
                pltpu.VMEM((2 * half_ff, width), BF16),
                pltpu.VMEM((IN_SLOTS, seq, width), BF16),
                pltpu.VMEM((OUT_SLOTS, seq, width), BF16),
                pltpu.VMEM((seq, width), BF16),
                pltpu.VMEM((seq, 3 * width), BF16),
                pltpu.VMEM((seq, width), BF16),
                pltpu.VMEM((seq, width), BF16),
                pltpu.VMEM((seq, 2 * half_ff), BF16),
                pltpu.SemaphoreType.DMA((8,)),
                pltpu.SemaphoreType.DMA((8,)),
                pltpu.SemaphoreType.DMA((8,)),
                pltpu.SemaphoreType.DMA((IN_SLOTS,)),
                pltpu.SemaphoreType.DMA((OUT_SLOTS,)),
                pltpu.SemaphoreType.DMA((OUT_SLOTS,)),
                pltpu.SemaphoreType.DMA((n_single,)),
                pltpu.SemaphoreType.DMA((n_single,)),
                pltpu.SemaphoreType.REGULAR,
                pltpu.SemaphoreType.REGULAR,
            ],
            compiler_params=pltpu.CompilerParams(
                collective_id=0, has_side_effects=True, vmem_limit_bytes=60 * 2**20
            ),
        )(*operands)
        return out.reshape(1, micro, rows, seq, width)

    return jax.shard_map(
        local_run,
        mesh=mesh,
        in_specs=(P(None, "dp", None, None),) + weight_specs,
        out_specs=P("pp", None, "dp", None, None),
        check_vma=False,
    )
```

```python
import functools
import math

import jax
import jax.numpy as jnp
from jax import lax
from jax.experimental import pallas as pl
from jax.experimental.pallas import tpu as pltpu
from jax.sharding import PartitionSpec as P

F32 = jnp.float32
BF16 = jnp.bfloat16
MESH = pl.DeviceIdType.MESH
LN_EPS = 1e-5
N_DUP = 18
IN_SLOTS = 3
OUT_SLOTS = 2
QUERY_BLOCK = 256
COL_BLOCK = 256
ROW_BLOCK = 128
GELU_C0 = math.sqrt(2.0 / math.pi)
GELU_C1 = GELU_C0 * 0.044715


def dot(a, b, ca=1, cb=0):
    return lax.dot_general(a, b, (((ca,), (cb,)), ((), ())), preferred_element_type=F32)


def layer_norm(x, gain, bias):
    x = x.astype(F32)
    mean = jnp.mean(x, axis=-1, keepdims=True)
    centered = x - mean
    var = jnp.mean(centered * centered, axis=-1, keepdims=True)
    return (centered * lax.rsqrt(var + LN_EPS) * gain.astype(F32) + bias.astype(F32)).astype(BF16)


def gelu(z):
    return z * jax.nn.sigmoid(z * (2.0 * GELU_C0 + 2.0 * GELU_C1 * (z * z)))


def attention(qkv, ctx, head_dim):
    seq, width = ctx.shape
    pair = 2 * head_dim
    scale = head_dim**-0.5 * math.log2(math.e)
    first = lax.broadcasted_iota(jnp.int32, (1, pair), 1) < head_dim
    zero = jnp.zeros((), BF16)
    block = QUERY_BLOCK
    keep = lax.broadcasted_iota(jnp.int32, (block, block), 0) >= lax.broadcasted_iota(jnp.int32, (block, block), 1)
    keep = jnp.concatenate([keep, keep], axis=0)
    for q0 in range(seq - block, -1, -block):
        for p in range(width // pair):
            lanes = slice(p * pair, (p + 1) * pair)
            keys = qkv[: q0 + block, width + p * pair : width + (p + 1) * pair]
            values = qkv[: q0 + block, 2 * width + p * pair : 2 * width + (p + 1) * pair]
            q = qkv[q0 : q0 + block, lanes]
            q = jnp.concatenate([jnp.where(first, q, zero), jnp.where(first, zero, q)], axis=0)
            scores = dot(q, keys, 1, 1)
            diag = jnp.where(keep, scores[:, q0:], -1e30)
            scores = jnp.concatenate([scores[:, :q0], diag], axis=1) if q0 else diag
            top = jnp.max(scores, axis=-1, keepdims=True)
            probs = jnp.exp2((scores - top) * scale)
            total = jnp.sum(probs, axis=-1, keepdims=True)
            out = dot(probs.astype(BF16), values) * (1.0 / total)
            ctx[q0 : q0 + block, lanes] = jnp.where(first, out[:block], out[block:]).astype(BF16)


def project_residual(lhs, weight, bias, resid, out, rows):
    for n in range(0, out.shape[1], COL_BLOCK):
        cols = slice(n, n + COL_BLOCK)
        part = (dot(lhs[rows], weight[:, cols]) + bias[:, cols].astype(F32)).astype(BF16)
        out[rows, cols] = (resid[rows, cols].astype(F32) + part.astype(F32)).astype(BF16)


def one_layer(x, y, w, s, head_dim, between):
    seq, width = x.shape
    blocks = [slice(m, m + ROW_BLOCK) for m in range(0, seq, ROW_BLOCK)]
    for rows in blocks:
        s["h"][rows] = layer_norm(x[rows], w["g1"][...], w["c1"][...])
        for n in range(0, 3 * width, COL_BLOCK):
            cols = slice(n, n + COL_BLOCK)
            s["qkv"][rows, cols] = (dot(s["h"][rows], w["qkv"][:, cols]) + w["bqkv"][:, cols]).astype(BF16)
    between()
    attention(s["qkv"], s["ctx"], head_dim)
    for rows in blocks:
        project_residual(s["ctx"], w["out"], w["bout"], x, s["x1"], rows)
        s["h"][rows] = layer_norm(s["x1"][rows], w["g2"][...], w["c2"][...])
    half = w["up"].shape[2]
    for t in range(2):
        for n in range(0, half, COL_BLOCK):
            for rows in blocks:
                z = dot(s["h"][rows], w["up"][t, :, n : n + COL_BLOCK])
                z = z + w["bup"][t, :, n : n + COL_BLOCK].astype(F32)
                s["u"][rows, t * half + n : t * half + n + COL_BLOCK] = gelu(z).astype(BF16)
    for n in range(0, width, COL_BLOCK):
        for rows in blocks:
            cols = slice(n, n + COL_BLOCK)
            part = (dot(s["u"][rows], w["down"][:, cols]) + w["bdown"][:, cols].astype(F32)).astype(BF16)
            y[rows, cols] = (s["x1"][rows, cols].astype(F32) + part.astype(F32)).astype(BF16)


def kernel(
    cfg,
    x_hbm, g1, c1, bout, g2, c2, bdown, qkv_half, bqkv_half, out_half, up_half, bup_half, down_half,
    out_hbm,
    w_qkv_raw, w_qkv, b_qkv_raw, b_qkv, w_out, w_up, b_up, w_down,
    x_in, y_out, h, qkv, ctx, x1, u,
    w_local, w_send, w_recv, in_sem, store_sem, hop_sem, side_send, side_recv, credit, turn,
):
    stages, n_single, n_dup, head_dim = cfg
    total = n_single + n_dup
    t = lax.axis_index("tp")
    p = lax.axis_index("pp")
    width = x_hbm.shape[2]
    half_width = width // 2
    other = {"tp": 1 - t}
    after = {"pp": lax.rem(p + 1, stages)}
    before = {"pp": lax.rem(p + stages - 1, stages)}

    barrier = pltpu.get_barrier_semaphore()
    for peer in (other, after, before):
        pl.semaphore_signal(barrier, inc=1, device_id=peer, device_id_type=MESH)
    pl.semaphore_wait(barrier, 3)

    half_ff = down_half.shape[0]
    mine = pl.ds(pl.multiple_of(t * half_width, 128), half_width)
    pieces = [(qkv_half.at[c], w_qkv_raw.at[c, mine]) for c in range(3)]
    pieces.append((bqkv_half, b_qkv_raw.at[t]))
    pieces.append((out_half, w_out.at[mine]))
    pieces.append((bup_half, b_up.at[t]))
    pieces.append((up_half, w_up.at[t]))
    pieces.append((down_half, w_down.at[pl.ds(pl.multiple_of(t * half_ff, 128), half_ff)]))
    near, far = [], []
    for i, (src, dst) in enumerate(pieces):
        near.append(pltpu.make_async_copy(src, dst, w_local.at[i]))
        far.append(
            pltpu.make_async_remote_copy(src, dst, w_send.at[i], w_recv.at[i], device_id=other, device_id_type=MESH)
        )
        near[-1].start()

    @pl.when(lax.rem(p, 2) == 1)
    def _():
        pl.semaphore_wait(turn, 1)

    for copy in far:
        copy.start()

    def dups_before(n):
        return n * n_dup // total

    def single_index(n):
        return n - dups_before(n)

    def is_dup(n):
        return dups_before(n + 1) - dups_before(n)

    def row_of(n):
        dup = is_dup(n)
        return dup * (2 * n_single + dups_before(n)) + (1 - dup) * (t * n_single + single_index(n))

    def load(n):
        slot = lax.rem(n, IN_SLOTS)
        return pltpu.make_async_copy(x_hbm.at[row_of(n)], x_in.at[slot], in_sem.at[slot])

    def store(n):
        slot = lax.rem(n, OUT_SLOTS)
        return pltpu.make_async_copy(y_out.at[slot], out_hbm.at[row_of(n)], store_sem.at[slot])

    def hop(n):
        src, dst = lax.rem(n, OUT_SLOTS), lax.rem(n, IN_SLOTS)
        return pltpu.make_async_remote_copy(
            y_out.at[src], x_in.at[dst], hop_sem.at[src], in_sem.at[dst], device_id=after, device_id_type=MESH
        )

    def side(k):
        row = t * n_single + k
        return pltpu.make_async_remote_copy(
            out_hbm.at[row], out_hbm.at[row], side_send.at[k], side_recv.at[k], device_id=other, device_id_type=MESH
        )

    @pl.when(p == 0)
    def _():
        load(0).start()

    def arrived(i):
        near[i].wait()
        far[i].wait_recv()

    for i in range(4):
        arrived(i)
    for c in range(3):
        for m in range(0, width, COL_BLOCK):
            w_qkv[:, c * width + m : c * width + m + COL_BLOCK] = w_qkv_raw[c, m : m + COL_BLOCK, :].T
        for k in range(2):
            for head in range(half_width // head_dim):
                at = c * width + k * half_width + head * head_dim
                b_qkv[:, at : at + head_dim] = b_qkv_raw[k, c, head : head + 1, :].astype(F32)
    for copy in far[:6]:
        copy.wait_send()

    @pl.when(lax.rem(p, 2) == 0)
    def _():
        pl.semaphore_signal(turn, inc=1, device_id=after, device_id_type=MESH)

    for i in range(4, len(far)):
        arrived(i)

    weights = dict(
        g1=g1, c1=c1, qkv=w_qkv, bqkv=b_qkv, out=w_out, bout=bout, g2=g2, c2=c2,
        up=w_up, bup=b_up, down=w_down, bdown=bdown,
    )
    scratch = dict(h=h, qkv=qkv, ctx=ctx, x1=x1, u=u)

    def publish(n):
        store(n).wait()

        @pl.when(is_dup(n) == 0)
        def _():
            side(single_index(n)).start()

    def step(n, carry):
        in_slot, out_slot = lax.rem(n, IN_SLOTS), lax.rem(n, OUT_SLOTS)
        load(n).wait()

        @pl.when((p == 0) & (n + 1 < total))
        def _():
            load(n + 1).start()

        @pl.when((n >= OUT_SLOTS) & (p < stages - 1))
        def _():
            hop(n - OUT_SLOTS).wait_send()

        def between():
            @pl.when(n >= 1)
            def _():
                publish(n - 1)

        one_layer(x_in.at[in_slot], y_out.at[out_slot], weights, scratch, head_dim, between)

        store(n).start()

        @pl.when((p < stages - 1) & (n >= IN_SLOTS))
        def _():
            pl.semaphore_wait(credit, 1)

        @pl.when(p < stages - 1)
        def _():
            hop(n).start()

        @pl.when((p > 0) & (n + IN_SLOTS < total))
        def _():
            pl.semaphore_signal(credit, inc=1, device_id=before, device_id_type=MESH)

        return carry

    lax.fori_loop(0, total, step, 0)
    publish(total - 1)

    @pl.when(p < stages - 1)
    def _():
        for n in range(total - OUT_SLOTS, total):
            hop(n).wait_send()

    for copy in far[6:]:
        copy.wait_send()

    def finish(k, carry):
        side(k).wait_send()
        side(k).wait_recv()
        return carry

    lax.fori_loop(0, n_single, finish, 0)


def solution(mesh):
    stages = mesh.shape["pp"]
    weight_specs = (
        P("pp", None), P("pp", None),
        P("pp", None, None, "tp", None), P("pp", None, "tp", None),
        P("pp", "tp", None, None), P("pp", None),
        P("pp", None), P("pp", None),
        P("pp", None, "tp"), P("pp", "tp"),
        P("pp", "tp", None), P("pp", None),
    )

    def local_run(x_micro, g1, c1, w_qkv, b_qkv, w_out, b_out, g2, c2, w_up, b_up, w_down, b_down):
        micro, rows, seq, width = x_micro.shape
        count = micro * rows
        heads, head_dim = w_qkv.shape[3:]
        half_width = heads * head_dim
        half_ff = w_up.shape[2]
        n_dup = N_DUP
        n_single = (count - n_dup) // 2
        cfg = (stages, n_single, n_dup, head_dim)
        operands = (
            x_micro.reshape(count, seq, width),
            g1, c1, b_out, g2, c2, b_down,
            w_qkv.reshape(3, width, heads, head_dim).transpose(0, 2, 3, 1).reshape(3, half_width, width),
            b_qkv.reshape(3, heads, head_dim),
            w_out.reshape(half_width, width),
            w_up.reshape(width, half_ff),
            b_up.reshape(1, half_ff),
            w_down.reshape(half_ff, width),
        )
        anywhere = pl.BlockSpec(memory_space=pl.ANY)
        vmem = pl.BlockSpec(memory_space=pltpu.VMEM)
        out = pl.pallas_call(
            functools.partial(kernel, cfg),
            out_shape=jax.ShapeDtypeStruct((count, seq, width), BF16),
            in_specs=[anywhere] + [vmem] * 6 + [anywhere] * 6,
            out_specs=anywhere,
            scratch_shapes=[
                pltpu.VMEM((3, width, width), BF16),
                pltpu.VMEM((width, 3 * width), BF16),
                pltpu.VMEM((2, 3, heads, head_dim), BF16),
                pltpu.VMEM((1, 3 * width), F32),
                pltpu.VMEM((width, width), BF16),
                pltpu.VMEM((2, width, half_ff), BF16),
                pltpu.VMEM((2, 1, half_ff), BF16),
                pltpu.VMEM((2 * half_ff, width), BF16),
                pltpu.VMEM((IN_SLOTS, seq, width), BF16),
                pltpu.VMEM((OUT_SLOTS, seq, width), BF16),
                pltpu.VMEM((seq, width), BF16),
                pltpu.VMEM((seq, 3 * width), BF16),
                pltpu.VMEM((seq, width), BF16),
                pltpu.VMEM((seq, width), BF16),
                pltpu.VMEM((seq, 2 * half_ff), BF16),
                pltpu.SemaphoreType.DMA((8,)),
                pltpu.SemaphoreType.DMA((8,)),
                pltpu.SemaphoreType.DMA((8,)),
                pltpu.SemaphoreType.DMA((IN_SLOTS,)),
                pltpu.SemaphoreType.DMA((OUT_SLOTS,)),
                pltpu.SemaphoreType.DMA((OUT_SLOTS,)),
                pltpu.SemaphoreType.DMA((n_single,)),
                pltpu.SemaphoreType.DMA((n_single,)),
                pltpu.SemaphoreType.REGULAR,
                pltpu.SemaphoreType.REGULAR,
            ],
            compiler_params=pltpu.CompilerParams(
                collective_id=0, has_side_effects=True, vmem_limit_bytes=60 * 2**20
            ),
        )(*operands)
        return out.reshape(1, micro, rows, seq, width)

    return jax.shard_map(
        local_run,
        mesh=mesh,
        in_specs=(P(None, "dp", None, None),) + weight_specs,
        out_specs=P("pp", None, "dp", None, None),
        check_vma=False,
    )
```

```python
import functools
import math

import jax
import jax.numpy as jnp
from jax import lax
from jax.experimental import pallas as pl
from jax.experimental.pallas import tpu as pltpu
from jax.sharding import PartitionSpec as P

F32 = jnp.float32
BF16 = jnp.bfloat16
MESH = pl.DeviceIdType.MESH
LN_EPS = 1e-5
N_DUP = 20
IN_SLOTS = 3
OUT_SLOTS = 4
QUERY_BLOCK = 256
COL_BLOCK = 768
ROW_BLOCK = 128
MID_ROW_BLOCK = 256
GELU_C0 = math.sqrt(2.0 / math.pi)
GELU_C1 = GELU_C0 * 0.044715


def dot(a, b, ca=1, cb=0):
    return lax.dot_general(a, b, (((ca,), (cb,)), ((), ())), preferred_element_type=F32)


def layer_norm(x, gain, bias):
    x = x.astype(F32)
    mean = jnp.mean(x, axis=-1, keepdims=True)
    centered = x - mean
    var = jnp.mean(centered * centered, axis=-1, keepdims=True)
    return (centered * lax.rsqrt(var + LN_EPS) * gain.astype(F32) + bias.astype(F32)).astype(BF16)


def gelu(z):
    return z * jax.nn.sigmoid(z * (2.0 * GELU_C0 + 2.0 * GELU_C1 * (z * z)))


def attention(qkv, ctx, head_dim):
    seq, width = ctx.shape
    pair = 2 * head_dim
    scale = head_dim**-0.5 * math.log2(math.e)
    first = lax.broadcasted_iota(jnp.int32, (1, pair), 1) < head_dim
    zero = jnp.zeros((), BF16)
    block = QUERY_BLOCK
    keep = lax.broadcasted_iota(jnp.int32, (block, block), 0) >= lax.broadcasted_iota(jnp.int32, (block, block), 1)
    keep = jnp.concatenate([keep, keep], axis=0)
    for q0 in range(seq - block, -1, -block):
        for p in range(width // pair):
            lanes = slice(p * pair, (p + 1) * pair)
            keys = qkv[: q0 + block, width + p * pair : width + (p + 1) * pair]
            values = qkv[: q0 + block, 2 * width + p * pair : 2 * width + (p + 1) * pair]
            q = qkv[q0 : q0 + block, lanes]
            q = jnp.concatenate([jnp.where(first, q, zero), jnp.where(first, zero, q)], axis=0)
            scores = dot(q, keys, 1, 1)
            diag = jnp.where(keep, scores[:, q0:], -1e30)
            scores = jnp.concatenate([scores[:, :q0], diag], axis=1) if q0 else diag
            top = jnp.max(scores, axis=-1, keepdims=True)
            probs = jnp.exp2((scores - top) * scale)
            total = jnp.sum(probs, axis=-1, keepdims=True)
            out = dot(probs.astype(BF16), values) * (1.0 / total)
            ctx[q0 : q0 + block, lanes] = jnp.where(first, out[:block], out[block:]).astype(BF16)


def col_blocks(size):
    block = min(COL_BLOCK, size)
    return [slice(n, n + block) for n in range(0, size, block)]


def project_residual(lhs, weight, bias, resid, out, rows, cols):
    part = (dot(lhs[rows], weight[:, cols]) + bias[:, cols].astype(F32)).astype(BF16)
    out[rows, cols] = (resid[rows, cols].astype(F32) + part.astype(F32)).astype(BF16)


def one_layer(x, y, w, s, head_dim):
    seq, width = x.shape
    blocks = [slice(m, m + ROW_BLOCK) for m in range(0, seq, ROW_BLOCK)]
    for rows in blocks:
        s["h"][rows] = layer_norm(x[rows], w["g1"][...], w["c1"][...])
        for cols in col_blocks(3 * width):
            s["qkv"][rows, cols] = (dot(s["h"][rows], w["qkv"][:, cols]) + w["bqkv"][:, cols]).astype(BF16)
    attention(s["qkv"], s["ctx"], head_dim)
    for m in range(0, seq, MID_ROW_BLOCK):
        rows = slice(m, m + MID_ROW_BLOCK)
        for cols in col_blocks(width):
            project_residual(s["ctx"], w["out"], w["bout"], x, s["x1"], rows, cols)
        s["h"][rows] = layer_norm(s["x1"][rows], w["g2"][...], w["c2"][...])
    half = w["up"].shape[2]
    for t in range(2):
        for cols in col_blocks(half):
            for rows in blocks:
                z = dot(s["h"][rows], w["up"][t, :, cols]) + w["bup"][t, :, cols].astype(F32)
                s["u"][rows, t * half + cols.start : t * half + cols.stop] = gelu(z).astype(BF16)
    for cols in col_blocks(width):
        for rows in blocks:
            project_residual(s["u"], w["down"], w["bdown"], s["x1"], y, rows, cols)


def kernel(
    cfg,
    x_hbm, g1, c1, bout, g2, c2, bdown, qkv_half, bqkv_half, out_half, up_half, bup_half, down_half,
    out_hbm,
    w_qkv_raw, w_qkv, b_qkv_raw, b_qkv, w_out, w_up, b_up, w_down,
    relay_a, relay_b, x_in, y_out, h, qkv, ctx, x1, u,
    w_local, w_send, w_recv, r_send, r_recv, in_sem, store_sem, hop_sem, side_send, side_recv, credit, turn,
):
    stages, n_single, n_dup, head_dim = cfg
    total = n_single + n_dup
    t = lax.axis_index("tp")
    p = lax.axis_index("pp")
    width = x_hbm.shape[2]
    half_width = width // 2
    other = {"tp": 1 - t}
    after = {"pp": lax.rem(p + 1, stages)}
    before = {"pp": lax.rem(p + stages - 1, stages)}

    across = {"pp": lax.rem(p + 2, stages)}

    barrier = pltpu.get_barrier_semaphore()
    for peer in (other, after, before, across):
        pl.semaphore_signal(barrier, inc=1, device_id=peer, device_id_type=MESH)
    pl.semaphore_wait(barrier, 4)

    half_ff = down_half.shape[0]
    mine = pl.ds(pl.multiple_of(t * half_width, 128), half_width)
    pieces = [(qkv_half.at[c], w_qkv_raw.at[c, mine]) for c in range(3)]
    pieces.append((bqkv_half, b_qkv_raw.at[t]))
    pieces.append((out_half, w_out.at[mine]))
    pieces.append((bup_half, b_up.at[t]))
    pieces.append((up_half, w_up.at[t]))
    relayed = relay_a.shape[0]
    direct = half_ff - relayed
    down_at = pl.multiple_of(t * half_ff, 128)
    pieces.append((down_half.at[:direct], w_down.at[pl.ds(down_at, direct)]))
    pieces.append((down_half.at[direct:], w_down.at[pl.ds(down_at + direct, relayed)]))
    near, far = [], []
    for i, (src, dst) in enumerate(pieces):
        near.append(pltpu.make_async_copy(src, dst, w_local.at[i]))
        far.append(
            pltpu.make_async_remote_copy(src, dst, w_send.at[i], w_recv.at[i], device_id=other, device_id_type=MESH)
        )
        near[-1].start()

    last = len(pieces) - 1
    far_down_at = pl.multiple_of((1 - t) * half_ff, 128)
    relay = [
        pltpu.make_async_remote_copy(src, dst, r_send.at[i], r_recv.at[i], device_id=to, device_id_type=MESH)
        for i, (src, dst, to) in enumerate(
            [(down_half.at[direct:], relay_a, across), (relay_a, relay_b, other)]
        )
    ]
    relay.append(
        pltpu.make_async_remote_copy(
            relay_b, w_down.at[pl.ds(far_down_at + direct, relayed)], r_send.at[2], w_recv.at[last],
            device_id=across, device_id_type=MESH,
        )
    )

    @pl.when(p == 1)
    def _():
        relay[0].start()

    @pl.when(p == 3)
    def _():
        relay[0].wait_recv()
        relay[1].start()
        relay[1].wait_recv()
        relay[2].start()

    @pl.when(lax.rem(p, 2) == 1)
    def _():
        pl.semaphore_wait(turn, 1)

    for copy in far[:last]:
        copy.start()

    @pl.when(p != 1)
    def _():
        far[last].start()

    def dups_before(n):
        return n * n_dup // total

    def single_index(n):
        return n - dups_before(n)

    def is_dup(n):
        return dups_before(n + 1) - dups_before(n)

    def row_of(n):
        dup = is_dup(n)
        return dup * (2 * n_single + dups_before(n)) + (1 - dup) * (t * n_single + single_index(n))

    def load(n):
        slot = lax.rem(n, IN_SLOTS)
        return pltpu.make_async_copy(x_hbm.at[row_of(n)], x_in.at[slot], in_sem.at[slot])

    def store(n):
        slot = lax.rem(n, OUT_SLOTS)
        return pltpu.make_async_copy(y_out.at[slot], out_hbm.at[row_of(n)], store_sem.at[slot])

    def hop(n):
        src, dst = lax.rem(n, OUT_SLOTS), lax.rem(n, IN_SLOTS)
        return pltpu.make_async_remote_copy(
            y_out.at[src], x_in.at[dst], hop_sem.at[src], in_sem.at[dst], device_id=after, device_id_type=MESH
        )

    def side(n):
        slot, k = lax.rem(n, OUT_SLOTS), single_index(n)
        return pltpu.make_async_remote_copy(
            y_out.at[slot], out_hbm.at[t * n_single + k], side_send.at[k], side_recv.at[k],
            device_id=other, device_id_type=MESH,
        )

    def reuse(n):
        store(n).wait()

        @pl.when(p < stages - 1)
        def _():
            hop(n).wait_send()

        @pl.when(is_dup(n) == 0)
        def _():
            side(n).wait_send()

    @pl.when(p == 0)
    def _():
        load(0).start()

    def arrived(i):
        near[i].wait()
        far[i].wait_recv()

    for i in range(4):
        arrived(i)
    for c in range(3):
        for m in range(0, width, QUERY_BLOCK):
            w_qkv[:, c * width + m : c * width + m + QUERY_BLOCK] = w_qkv_raw[c, m : m + QUERY_BLOCK, :].T
        for k in range(2):
            for head in range(half_width // head_dim):
                at = c * width + k * half_width + head * head_dim
                b_qkv[:, at : at + head_dim] = b_qkv_raw[k, c, head : head + 1, :].astype(F32)
    for copy in far[:6]:
        copy.wait_send()

    @pl.when(lax.rem(p, 2) == 0)
    def _():
        pl.semaphore_signal(turn, inc=1, device_id=after, device_id_type=MESH)

    for i in range(4, len(far)):
        arrived(i)

    weights = dict(
        g1=g1, c1=c1, qkv=w_qkv, bqkv=b_qkv, out=w_out, bout=bout, g2=g2, c2=c2,
        up=w_up, bup=b_up, down=w_down, bdown=bdown,
    )
    scratch = dict(h=h, qkv=qkv, ctx=ctx, x1=x1, u=u)

    def step(n, carry):
        in_slot, out_slot = lax.rem(n, IN_SLOTS), lax.rem(n, OUT_SLOTS)
        load(n).wait()

        @pl.when((p == 0) & (n + 1 < total))
        def _():
            load(n + 1).start()

        @pl.when(n >= OUT_SLOTS)
        def _():
            reuse(n - OUT_SLOTS)

        one_layer(x_in.at[in_slot], y_out.at[out_slot], weights, scratch, head_dim)

        store(n).start()

        @pl.when((p < stages - 1) & (n >= IN_SLOTS))
        def _():
            pl.semaphore_wait(credit, 1)

        @pl.when(p < stages - 1)
        def _():
            hop(n).start()

        @pl.when(is_dup(n) == 0)
        def _():
            side(n).start()

        @pl.when((p > 0) & (n + IN_SLOTS < total))
        def _():
            pl.semaphore_signal(credit, inc=1, device_id=before, device_id_type=MESH)

        return carry

    lax.fori_loop(0, total, step, 0)
    def drain(n, carry):
        reuse(n)
        return carry

    lax.fori_loop(total - OUT_SLOTS, total, drain, 0)

    for copy in far[6:last]:
        copy.wait_send()

    @pl.when(p != 1)
    def _():
        far[last].wait_send()

    @pl.when(p == 1)
    def _():
        relay[0].wait_send()

    @pl.when(p == 3)
    def _():
        relay[1].wait_send()
        relay[2].wait_send()

    def finish(k, carry):
        row = (1 - t) * n_single + k
        pltpu.make_async_copy(out_hbm.at[row], out_hbm.at[row], side_recv.at[k]).wait()
        return carry

    lax.fori_loop(0, n_single, finish, 0)


def solution(mesh):
    stages = mesh.shape["pp"]
    weight_specs = (
        P("pp", None), P("pp", None),
        P("pp", None, None, "tp", None), P("pp", None, "tp", None),
        P("pp", "tp", None, None), P("pp", None),
        P("pp", None), P("pp", None),
        P("pp", None, "tp"), P("pp", "tp"),
        P("pp", "tp", None), P("pp", None),
    )

    def local_run(x_micro, g1, c1, w_qkv, b_qkv, w_out, b_out, g2, c2, w_up, b_up, w_down, b_down):
        micro, rows, seq, width = x_micro.shape
        count = micro * rows
        heads, head_dim = w_qkv.shape[3:]
        half_width = heads * head_dim
        half_ff = w_up.shape[2]
        relayed = 2 * half_ff // 3 // 128 * 128
        n_dup = N_DUP
        n_single = (count - n_dup) // 2
        cfg = (stages, n_single, n_dup, head_dim)
        operands = (
            x_micro.reshape(count, seq, width),
            g1, c1, b_out, g2, c2, b_down,
            w_qkv.reshape(3, width, heads, head_dim).transpose(0, 2, 3, 1).reshape(3, half_width, width),
            b_qkv.reshape(3, heads, head_dim),
            w_out.reshape(half_width, width),
            w_up.reshape(width, half_ff),
            b_up.reshape(1, half_ff),
            w_down.reshape(half_ff, width),
        )
        anywhere = pl.BlockSpec(memory_space=pl.ANY)
        vmem = pl.BlockSpec(memory_space=pltpu.VMEM)
        out = pl.pallas_call(
            functools.partial(kernel, cfg),
            out_shape=jax.ShapeDtypeStruct((count, seq, width), BF16),
            in_specs=[anywhere] + [vmem] * 6 + [anywhere] * 6,
            out_specs=anywhere,
            scratch_shapes=[
                pltpu.VMEM((3, width, width), BF16),
                pltpu.VMEM((width, 3 * width), BF16),
                pltpu.VMEM((2, 3, heads, head_dim), BF16),
                pltpu.VMEM((1, 3 * width), F32),
                pltpu.VMEM((width, width), BF16),
                pltpu.VMEM((2, width, half_ff), BF16),
                pltpu.VMEM((2, 1, half_ff), BF16),
                pltpu.VMEM((2 * half_ff, width), BF16),
                pltpu.VMEM((relayed, width), BF16),
                pltpu.VMEM((relayed, width), BF16),
                pltpu.VMEM((IN_SLOTS, seq, width), BF16),
                pltpu.VMEM((OUT_SLOTS, seq, width), BF16),
                pltpu.VMEM((seq, width), BF16),
                pltpu.VMEM((seq, 3 * width), BF16),
                pltpu.VMEM((seq, width), BF16),
                pltpu.VMEM((seq, width), BF16),
                pltpu.VMEM((seq, 2 * half_ff), BF16),
                pltpu.SemaphoreType.DMA((9,)),
                pltpu.SemaphoreType.DMA((9,)),
                pltpu.SemaphoreType.DMA((9,)),
                pltpu.SemaphoreType.DMA((3,)),
                pltpu.SemaphoreType.DMA((2,)),
                pltpu.SemaphoreType.DMA((IN_SLOTS,)),
                pltpu.SemaphoreType.DMA((OUT_SLOTS,)),
                pltpu.SemaphoreType.DMA((OUT_SLOTS,)),
                pltpu.SemaphoreType.DMA((n_single,)),
                pltpu.SemaphoreType.DMA((n_single,)),
                pltpu.SemaphoreType.REGULAR,
                pltpu.SemaphoreType.REGULAR,
            ],
            compiler_params=pltpu.CompilerParams(
                collective_id=0,
                has_side_effects=True,
                vmem_limit_bytes=60 * 2**20,
            ),
        )(*operands)
        return out.reshape(1, micro, rows, seq, width)

    return jax.shard_map(
        local_run,
        mesh=mesh,
        in_specs=(P(None, "dp", None, None),) + weight_specs,
        out_specs=P("pp", None, "dp", None, None),
        check_vma=False,
    )
```

```python
import functools
import math

import jax
import jax.numpy as jnp
from jax import lax
from jax.experimental import pallas as pl
from jax.experimental.pallas import tpu as pltpu
from jax.sharding import PartitionSpec as P

F32 = jnp.float32
BF16 = jnp.bfloat16
MESH = pl.DeviceIdType.MESH
LN_EPS = 1e-5
N_DUP = 16
N_LATE = 3
IN_SLOTS = 3
OUT_SLOTS = 4
QUERY_BLOCK = 256
COL_BLOCK = 768
ROW_BLOCK = 128
MID_ROW_BLOCK = 256
COPY_ROWS = 3
COPY_SLOTS = 16
GELU_C0 = math.sqrt(2.0 / math.pi)
GELU_C1 = GELU_C0 * 0.044715


def dot(a, b, ca=1, cb=0):
    return lax.dot_general(a, b, (((ca,), (cb,)), ((), ())), preferred_element_type=F32)


def layer_norm(x, gain, bias):
    x = x.astype(F32)
    mean = jnp.mean(x, axis=-1, keepdims=True)
    centered = x - mean
    var = jnp.mean(centered * centered, axis=-1, keepdims=True)
    return (centered * lax.rsqrt(var + LN_EPS) * gain.astype(F32) + bias.astype(F32)).astype(BF16)


def gelu(z):
    return z * jax.nn.sigmoid(z * (2.0 * GELU_C0 + 2.0 * GELU_C1 * (z * z)))


def attention(qkv, ctx, head_dim):
    seq, width = ctx.shape
    pair = 2 * head_dim
    scale = head_dim**-0.5 * math.log2(math.e)
    first = lax.broadcasted_iota(jnp.int32, (1, pair), 1) < head_dim
    zero = jnp.zeros((), BF16)
    block = QUERY_BLOCK
    keep = lax.broadcasted_iota(jnp.int32, (block, block), 0) >= lax.broadcasted_iota(jnp.int32, (block, block), 1)
    keep = jnp.concatenate([keep, keep], axis=0)
    for q0 in range(seq - block, -1, -block):
        for p in range(width // pair):
            lanes = slice(p * pair, (p + 1) * pair)
            keys = qkv[: q0 + block, width + p * pair : width + (p + 1) * pair]
            values = qkv[: q0 + block, 2 * width + p * pair : 2 * width + (p + 1) * pair]
            q = qkv[q0 : q0 + block, lanes]
            q = jnp.concatenate([jnp.where(first, q, zero), jnp.where(first, zero, q)], axis=0)
            scores = dot(q, keys, 1, 1)
            diag = jnp.where(keep, scores[:, q0:], -1e30)
            scores = jnp.concatenate([scores[:, :q0], diag], axis=1) if q0 else diag
            top = jnp.max(scores, axis=-1, keepdims=True)
            probs = jnp.exp2((scores - top) * scale)
            total = jnp.sum(probs, axis=-1, keepdims=True)
            out = dot(probs.astype(BF16), values) * (1.0 / total)
            ctx[q0 : q0 + block, lanes] = jnp.where(first, out[:block], out[block:]).astype(BF16)


def col_blocks(size):
    block = min(COL_BLOCK, size)
    return [slice(n, n + block) for n in range(0, size, block)]


def project_residual(lhs, weight, bias, resid, out, rows, cols):
    part = (dot(lhs[rows], weight[:, cols]) + bias[:, cols].astype(F32)).astype(BF16)
    out[rows, cols] = (resid[rows, cols].astype(F32) + part.astype(F32)).astype(BF16)


def one_layer(x, y, w, s, head_dim):
    seq, width = x.shape
    blocks = [slice(m, m + ROW_BLOCK) for m in range(0, seq, ROW_BLOCK)]
    for rows in blocks:
        s["h"][rows] = layer_norm(x[rows], w["g1"][...], w["c1"][...])
        for cols in col_blocks(3 * width):
            s["qkv"][rows, cols] = (dot(s["h"][rows], w["qkv"][:, cols]) + w["bqkv"][:, cols]).astype(BF16)
    attention(s["qkv"], s["ctx"], head_dim)
    for m in range(0, seq, MID_ROW_BLOCK):
        rows = slice(m, m + MID_ROW_BLOCK)
        for cols in col_blocks(width):
            project_residual(s["ctx"], w["out"], w["bout"], x, s["x1"], rows, cols)
        s["h"][rows] = layer_norm(s["x1"][rows], w["g2"][...], w["c2"][...])
    half = w["up"].shape[2]
    for t in range(2):
        for cols in col_blocks(half):
            for rows in blocks:
                z = dot(s["h"][rows], w["up"][t, :, cols]) + w["bup"][t, :, cols].astype(F32)
                s["u"][rows, t * half + cols.start : t * half + cols.stop] = gelu(z).astype(BF16)
    for cols in col_blocks(width):
        for rows in blocks:
            project_residual(s["u"], w["down"], w["bdown"], s["x1"], y, rows, cols)


def kernel(
    cfg,
    x_hbm, g1, c1, bout, g2, c2, bdown, qkv_half, bqkv_half, out_half, up_half, bup_half, down_half,
    out_hbm, late_hbm,
    w_qkv_raw, w_qkv, b_qkv_raw, b_qkv, w_out, w_up, b_up, w_down,
    relay_a, relay_b, x_in, y_out, h, qkv, ctx, x1, u,
    w_local, w_send, w_recv, r_send, r_recv, in_sem, store_sem, hop_sem, side_send, side_recv, credit, turn,
):
    stages, n_single, n_dup, head_dim = cfg
    n_early = n_single - late_hbm.shape[0]
    total = n_single + n_dup
    t = lax.axis_index("tp")
    p = lax.axis_index("pp")
    width = x_hbm.shape[2]
    half_width = width // 2
    other = {"tp": 1 - t}
    after = {"pp": lax.rem(p + 1, stages)}
    before = {"pp": lax.rem(p + stages - 1, stages)}

    across = {"pp": lax.rem(p + 2, stages)}

    barrier = pltpu.get_barrier_semaphore()
    for peer in (other, after, before, across):
        pl.semaphore_signal(barrier, inc=1, device_id=peer, device_id_type=MESH)
    pl.semaphore_wait(barrier, 4)

    half_ff = down_half.shape[0]
    mine = pl.ds(pl.multiple_of(t * half_width, 128), half_width)
    pieces = [(qkv_half.at[c], w_qkv_raw.at[c, mine]) for c in range(3)]
    pieces.append((bqkv_half, b_qkv_raw.at[t]))
    pieces.append((out_half, w_out.at[mine]))
    pieces.append((bup_half, b_up.at[t]))
    pieces.append((up_half, w_up.at[t]))
    relayed = relay_a.shape[0]
    direct = half_ff - relayed
    down_at = pl.multiple_of(t * half_ff, 128)
    pieces.append((down_half.at[:direct], w_down.at[pl.ds(down_at, direct)]))
    pieces.append((down_half.at[direct:], w_down.at[pl.ds(down_at + direct, relayed)]))
    near, far = [], []
    for i, (src, dst) in enumerate(pieces):
        near.append(pltpu.make_async_copy(src, dst, w_local.at[i]))
        far.append(
            pltpu.make_async_remote_copy(src, dst, w_send.at[i], w_recv.at[i], device_id=other, device_id_type=MESH)
        )
        near[-1].start()

    last = len(pieces) - 1
    far_down_at = pl.multiple_of((1 - t) * half_ff, 128)
    relay = [
        pltpu.make_async_remote_copy(src, dst, r_send.at[i], r_recv.at[i], device_id=to, device_id_type=MESH)
        for i, (src, dst, to) in enumerate(
            [(down_half.at[direct:], relay_a, across), (relay_a, relay_b, other)]
        )
    ]
    relay.append(
        pltpu.make_async_remote_copy(
            relay_b, w_down.at[pl.ds(far_down_at + direct, relayed)], r_send.at[2], w_recv.at[last],
            device_id=across, device_id_type=MESH,
        )
    )

    @pl.when(p == 1)
    def _():
        relay[0].start()

    @pl.when(p == 3)
    def _():
        relay[0].wait_recv()
        relay[1].start()
        relay[1].wait_recv()
        relay[2].start()

    @pl.when(lax.rem(p, 2) == 1)
    def _():
        pl.semaphore_wait(turn, 1)

    for copy in far[:last]:
        copy.start()

    @pl.when(p != 1)
    def _():
        far[last].start()

    def dups_before(n):
        return n * n_dup // total

    def single_index(n):
        return n - dups_before(n)

    def is_dup(n):
        return dups_before(n + 1) - dups_before(n)

    def row_of(n):
        dup = is_dup(n)
        return dup * (2 * n_single + dups_before(n)) + (1 - dup) * (t * n_single + single_index(n))

    def load(n):
        slot = lax.rem(n, IN_SLOTS)
        return pltpu.make_async_copy(x_hbm.at[row_of(n)], x_in.at[slot], in_sem.at[slot])

    def store(n):
        slot = lax.rem(n, OUT_SLOTS)
        return pltpu.make_async_copy(y_out.at[slot], out_hbm.at[row_of(n)], store_sem.at[slot])

    def hop(n):
        src, dst = lax.rem(n, OUT_SLOTS), lax.rem(n, IN_SLOTS)
        return pltpu.make_async_remote_copy(
            y_out.at[src], x_in.at[dst], hop_sem.at[src], in_sem.at[dst], device_id=after, device_id_type=MESH
        )

    def side(n):
        slot, k = lax.rem(n, OUT_SLOTS), single_index(n)
        return pltpu.make_async_remote_copy(
            y_out.at[slot], out_hbm.at[t * n_single + k], side_send.at[k], side_recv.at[k],
            device_id=other, device_id_type=MESH,
        )

    def keep_late(n):
        slot, k = lax.rem(n, OUT_SLOTS), single_index(n)
        return pltpu.make_async_copy(y_out.at[slot], late_hbm.at[k - n_early], side_send.at[k])

    def reuse(n):
        store(n).wait()

        @pl.when(p < stages - 1)
        def _():
            hop(n).wait_send()

        @pl.when((is_dup(n) == 0) & (single_index(n) < n_early))
        def _():
            side(n).wait_send()

        @pl.when((is_dup(n) == 0) & (single_index(n) >= n_early))
        def _():
            keep_late(n).wait()

    @pl.when(p == 0)
    def _():
        load(0).start()

    def arrived(i):
        near[i].wait()
        far[i].wait_recv()

    for i in range(4):
        arrived(i)
    for c in range(3):
        for m in range(0, width, QUERY_BLOCK):
            w_qkv[:, c * width + m : c * width + m + QUERY_BLOCK] = w_qkv_raw[c, m : m + QUERY_BLOCK, :].T
        for k in range(2):
            for head in range(half_width // head_dim):
                at = c * width + k * half_width + head * head_dim
                b_qkv[:, at : at + head_dim] = b_qkv_raw[k, c, head : head + 1, :].astype(F32)
    for copy in far[:6]:
        copy.wait_send()

    @pl.when(lax.rem(p, 2) == 0)
    def _():
        pl.semaphore_signal(turn, inc=1, device_id=after, device_id_type=MESH)

    for i in range(4, len(far)):
        arrived(i)

    weights = dict(
        g1=g1, c1=c1, qkv=w_qkv, bqkv=b_qkv, out=w_out, bout=bout, g2=g2, c2=c2,
        up=w_up, bup=b_up, down=w_down, bdown=bdown,
    )
    scratch = dict(h=h, qkv=qkv, ctx=ctx, x1=x1, u=u)

    def step(n, carry):
        in_slot, out_slot = lax.rem(n, IN_SLOTS), lax.rem(n, OUT_SLOTS)
        load(n).wait()

        @pl.when((p == 0) & (n + 1 < total))
        def _():
            load(n + 1).start()

        @pl.when(n >= OUT_SLOTS)
        def _():
            reuse(n - OUT_SLOTS)

        one_layer(x_in.at[in_slot], y_out.at[out_slot], weights, scratch, head_dim)

        store(n).start()

        @pl.when((p < stages - 1) & (n >= IN_SLOTS))
        def _():
            pl.semaphore_wait(credit, 1)

        @pl.when(p < stages - 1)
        def _():
            hop(n).start()

        @pl.when((is_dup(n) == 0) & (single_index(n) < n_early))
        def _():
            side(n).start()

        @pl.when((is_dup(n) == 0) & (single_index(n) >= n_early))
        def _():
            keep_late(n).start()

        @pl.when((p > 0) & (n + IN_SLOTS < total))
        def _():
            pl.semaphore_signal(credit, inc=1, device_id=before, device_id_type=MESH)

        return carry

    lax.fori_loop(0, total, step, 0)
    def drain(n, carry):
        reuse(n)
        return carry

    lax.fori_loop(total - OUT_SLOTS, total, drain, 0)

    for copy in far[6:last]:
        copy.wait_send()

    @pl.when(p != 1)
    def _():
        far[last].wait_send()

    @pl.when(p == 1)
    def _():
        relay[0].wait_send()

    @pl.when(p == 3)
    def _():
        relay[1].wait_send()
        relay[2].wait_send()

    def finish(k, carry):
        row = (1 - t) * n_single + k
        pltpu.make_async_copy(out_hbm.at[row], out_hbm.at[row], side_recv.at[k]).wait()
        return carry

    lax.fori_loop(0, n_early, finish, 0)


def copy_kernel(src, dst, held, sem_in, sem_out):
    slots = held.shape[0]
    steps = src.shape[0] // COPY_ROWS

    def rows(i):
        return pl.ds(i * COPY_ROWS, COPY_ROWS)

    def fetch(i):
        return pltpu.make_async_copy(src.at[rows(i)], held.at[i % slots], sem_in.at[i % slots])

    def put(i):
        return pltpu.make_async_copy(held.at[i % slots], dst.at[rows(i)], sem_out.at[i % slots])

    ahead = min(slots // 2, steps)
    for i in range(ahead):
        fetch(i).start()
    for i in range(steps):
        if i + ahead < steps:
            if i + ahead >= slots:
                put(i + ahead - slots).wait()
            fetch(i + ahead).start()
        fetch(i).wait()
        put(i).start()
    for i in range(max(steps - slots, 0), steps):
        put(i).wait()


def solution(mesh):
    stages = mesh.shape["pp"]
    weight_specs = (
        P("pp", None), P("pp", None),
        P("pp", None, None, "tp", None), P("pp", None, "tp", None),
        P("pp", "tp", None, None), P("pp", None),
        P("pp", None), P("pp", None),
        P("pp", None, "tp"), P("pp", "tp"),
        P("pp", "tp", None), P("pp", None),
    )

    def local_run(x_micro, g1, c1, w_qkv, b_qkv, w_out, b_out, g2, c2, w_up, b_up, w_down, b_down):
        micro, rows, seq, width = x_micro.shape
        count = micro * rows
        heads, head_dim = w_qkv.shape[3:]
        half_width = heads * head_dim
        half_ff = w_up.shape[2]
        relayed = 2 * half_ff // 3 // 128 * 128
        n_dup = N_DUP
        n_single = (count - n_dup) // 2
        cfg = (stages, n_single, n_dup, head_dim)
        operands = (
            x_micro.reshape(count, seq, width),
            g1, c1, b_out, g2, c2, b_down,
            w_qkv.reshape(3, width, heads, head_dim).transpose(0, 2, 3, 1).reshape(3, half_width, width),
            b_qkv.reshape(3, heads, head_dim),
            w_out.reshape(half_width, width),
            w_up.reshape(width, half_ff),
            b_up.reshape(1, half_ff),
            w_down.reshape(half_ff, width),
        )
        anywhere = pl.BlockSpec(memory_space=pl.ANY)
        vmem = pl.BlockSpec(memory_space=pltpu.VMEM)
        out, late = pl.pallas_call(
            functools.partial(kernel, cfg),
            out_shape=(
                jax.ShapeDtypeStruct((count, seq, width), BF16),
                jax.ShapeDtypeStruct((N_LATE, seq, width), BF16),
            ),
            in_specs=[anywhere] + [vmem] * 6 + [anywhere] * 6,
            out_specs=(anywhere, anywhere),
            scratch_shapes=[
                pltpu.VMEM((3, width, width), BF16),
                pltpu.VMEM((width, 3 * width), BF16),
                pltpu.VMEM((2, 3, heads, head_dim), BF16),
                pltpu.VMEM((1, 3 * width), F32),
                pltpu.VMEM((width, width), BF16),
                pltpu.VMEM((2, width, half_ff), BF16),
                pltpu.VMEM((2, 1, half_ff), BF16),
                pltpu.VMEM((2 * half_ff, width), BF16),
                pltpu.VMEM((relayed, width), BF16),
                pltpu.VMEM((relayed, width), BF16),
                pltpu.VMEM((IN_SLOTS, seq, width), BF16),
                pltpu.VMEM((OUT_SLOTS, seq, width), BF16),
                pltpu.VMEM((seq, width), BF16),
                pltpu.VMEM((seq, 3 * width), BF16),
                pltpu.VMEM((seq, width), BF16),
                pltpu.VMEM((seq, width), BF16),
                pltpu.VMEM((seq, 2 * half_ff), BF16),
                pltpu.SemaphoreType.DMA((9,)),
                pltpu.SemaphoreType.DMA((9,)),
                pltpu.SemaphoreType.DMA((9,)),
                pltpu.SemaphoreType.DMA((3,)),
                pltpu.SemaphoreType.DMA((2,)),
                pltpu.SemaphoreType.DMA((IN_SLOTS,)),
                pltpu.SemaphoreType.DMA((OUT_SLOTS,)),
                pltpu.SemaphoreType.DMA((OUT_SLOTS,)),
                pltpu.SemaphoreType.DMA((n_single,)),
                pltpu.SemaphoreType.DMA((n_single,)),
                pltpu.SemaphoreType.REGULAR,
                pltpu.SemaphoreType.REGULAR,
            ],
            compiler_params=pltpu.CompilerParams(
                collective_id=0,
                has_side_effects=True,
                vmem_limit_bytes=60 * 2**20,
            ),
        )(*operands)
        late = lax.ppermute(late, "tp", [(0, 1), (1, 0)])
        out = pl.pallas_call(
            copy_kernel,
            out_shape=jax.ShapeDtypeStruct((count, seq, width), BF16),
            in_specs=[anywhere],
            out_specs=anywhere,
            scratch_shapes=[
                pltpu.VMEM((COPY_SLOTS, COPY_ROWS, seq, width), BF16),
                pltpu.SemaphoreType.DMA((COPY_SLOTS,)),
                pltpu.SemaphoreType.DMA((COPY_SLOTS,)),
            ],
            compiler_params=pltpu.CompilerParams(vmem_limit_bytes=60 * 2**20),
            cost_estimate=pl.CostEstimate(
                flops=5 * 10**10, transcendentals=0, bytes_accessed=4 * count * seq * width
            ),
        )(out)
        first = (1 - lax.axis_index("tp")) * n_single + n_single - N_LATE
        out = lax.dynamic_update_slice(out, late, (first, 0, 0))
        return out.reshape(1, micro, rows, seq, width)

    return jax.shard_map(
        local_run,
        mesh=mesh,
        in_specs=(P(None, "dp", None, None),) + weight_specs,
        out_specs=P("pp", None, "dp", None, None),
        check_vma=False,
    )
```

```python
import functools
import math

import jax
import jax.numpy as jnp
from jax import lax
from jax.experimental import pallas as pl
from jax.experimental.pallas import tpu as pltpu
from jax.sharding import PartitionSpec as P

F32 = jnp.float32
BF16 = jnp.bfloat16
MESH = pl.DeviceIdType.MESH
LN_EPS = 1e-5
N_DUP = 16
N_LATE = 3
IN_SLOTS = 3
OUT_SLOTS = 6
HELD = 4
QUERY_BLOCK = 256
COL_BLOCK = 768
ROW_BLOCK = 128
MID_ROW_BLOCK = 256
COPY_SLOTS = 48
GELU_C0 = math.sqrt(2.0 / math.pi)
GELU_C1 = GELU_C0 * 0.044715


def dot(a, b, ca=1, cb=0):
    return lax.dot_general(a, b, (((ca,), (cb,)), ((), ())), preferred_element_type=F32)


def layer_norm(x, gain, bias):
    x = x.astype(F32)
    mean = jnp.mean(x, axis=-1, keepdims=True)
    centered = x - mean
    var = jnp.mean(centered * centered, axis=-1, keepdims=True)
    return (centered * lax.rsqrt(var + LN_EPS) * gain.astype(F32) + bias.astype(F32)).astype(BF16)


def gelu(z):
    return z * jax.nn.sigmoid(z * (2.0 * GELU_C0 + 2.0 * GELU_C1 * (z * z)))


def attention(qkv, ctx, head_dim):
    seq, width = ctx.shape
    pair = 2 * head_dim
    scale = head_dim**-0.5 * math.log2(math.e)
    first = lax.broadcasted_iota(jnp.int32, (1, pair), 1) < head_dim
    zero = jnp.zeros((), BF16)
    block = QUERY_BLOCK
    keep = lax.broadcasted_iota(jnp.int32, (block, block), 0) >= lax.broadcasted_iota(jnp.int32, (block, block), 1)
    keep = jnp.concatenate([keep, keep], axis=0)
    for q0 in range(seq - block, -1, -block):
        for p in range(width // pair):
            lanes = slice(p * pair, (p + 1) * pair)
            keys = qkv[: q0 + block, width + p * pair : width + (p + 1) * pair]
            values = qkv[: q0 + block, 2 * width + p * pair : 2 * width + (p + 1) * pair]
            q = qkv[q0 : q0 + block, lanes]
            q = jnp.concatenate([jnp.where(first, q, zero), jnp.where(first, zero, q)], axis=0)
            scores = dot(q, keys, 1, 1)
            diag = jnp.where(keep, scores[:, q0:], -1e30)
            scores = jnp.concatenate([scores[:, :q0], diag], axis=1) if q0 else diag
            top = jnp.max(scores, axis=-1, keepdims=True)
            probs = jnp.exp2((scores - top) * scale)
            total = jnp.sum(probs, axis=-1, keepdims=True)
            out = dot(probs.astype(BF16), values) * (1.0 / total)
            ctx[q0 : q0 + block, lanes] = jnp.where(first, out[:block], out[block:]).astype(BF16)


def col_blocks(size):
    block = min(COL_BLOCK, size)
    return [slice(n, n + block) for n in range(0, size, block)]


def project_residual(lhs, weight, bias, resid, out, rows, cols):
    part = (dot(lhs[rows], weight[:, cols]) + bias[:, cols].astype(F32)).astype(BF16)
    out[rows, cols] = (resid[rows, cols].astype(F32) + part.astype(F32)).astype(BF16)


def one_layer(x, y, w, s, head_dim):
    seq, width = x.shape
    blocks = [slice(m, m + ROW_BLOCK) for m in range(0, seq, ROW_BLOCK)]
    for rows in blocks:
        s["h"][rows] = layer_norm(x[rows], w["g1"][...], w["c1"][...])
        for cols in col_blocks(3 * width):
            s["qkv"][rows, cols] = (dot(s["h"][rows], w["qkv"][:, cols]) + w["bqkv"][:, cols]).astype(BF16)
    attention(s["qkv"], s["ctx"], head_dim)
    for m in range(0, seq, MID_ROW_BLOCK):
        rows = slice(m, m + MID_ROW_BLOCK)
        for cols in col_blocks(width):
            project_residual(s["ctx"], w["out"], w["bout"], x, s["x1"], rows, cols)
        s["h"][rows] = layer_norm(s["x1"][rows], w["g2"][...], w["c2"][...])
    half = w["up"].shape[2]
    for t in range(2):
        for cols in col_blocks(half):
            for rows in blocks:
                z = dot(s["h"][rows], w["up"][t, :, cols]) + w["bup"][t, :, cols].astype(F32)
                s["u"][rows, t * half + cols.start : t * half + cols.stop] = gelu(z).astype(BF16)
    for cols in col_blocks(width):
        for rows in blocks:
            project_residual(s["u"], w["down"], w["bdown"], s["x1"], y, rows, cols)


def kernel(
    cfg,
    x_hbm, g1, c1, bout, g2, c2, bdown, qkv_half, bqkv_half, out_half, up_half, bup_half, down_half,
    out_hbm, late_hbm,
    w_qkv_raw, w_qkv, b_qkv_raw, b_qkv, w_out, w_up, b_up, w_down,
    relay_a, relay_b, x_in, y_out, h, qkv, ctx, x1, u,
    w_local, w_send, w_recv, r_send, r_recv, in_sem, store_sem, hop_sem, side_send, side_recv, credit, turn, clear,
):
    stages, n_single, n_dup, head_dim = cfg
    n_early = n_single - late_hbm.shape[0]
    total = n_single + n_dup
    t = lax.axis_index("tp")
    p = lax.axis_index("pp")
    width = x_hbm.shape[2]
    half_width = width // 2
    other = {"tp": 1 - t}
    after = {"pp": lax.rem(p + 1, stages)}
    before = {"pp": lax.rem(p + stages - 1, stages)}

    across = {"pp": lax.rem(p + 2, stages)}

    barrier = pltpu.get_barrier_semaphore()
    for peer in (other, after, before, across):
        pl.semaphore_signal(barrier, inc=1, device_id=peer, device_id_type=MESH)
    pl.semaphore_wait(barrier, 4)

    half_ff = down_half.shape[0]
    mine = pl.ds(pl.multiple_of(t * half_width, 128), half_width)
    pieces = [(qkv_half.at[c], w_qkv_raw.at[c, mine]) for c in range(3)]
    pieces.append((bqkv_half, b_qkv_raw.at[t]))
    pieces.append((out_half, w_out.at[mine]))
    pieces.append((bup_half, b_up.at[t]))
    pieces.append((up_half, w_up.at[t]))
    relayed = relay_a.shape[0]
    direct = half_ff - relayed
    down_at = pl.multiple_of(t * half_ff, 128)
    pieces.append((down_half.at[:direct], w_down.at[pl.ds(down_at, direct)]))
    pieces.append((down_half.at[direct:], w_down.at[pl.ds(down_at + direct, relayed)]))
    near, far = [], []
    for i, (src, dst) in enumerate(pieces):
        near.append(pltpu.make_async_copy(src, dst, w_local.at[i]))
        far.append(
            pltpu.make_async_remote_copy(src, dst, w_send.at[i], w_recv.at[i], device_id=other, device_id_type=MESH)
        )
        near[-1].start()

    last = len(pieces) - 1
    far_down_at = pl.multiple_of((1 - t) * half_ff, 128)
    relay = [
        pltpu.make_async_remote_copy(src, dst, r_send.at[i], r_recv.at[i], device_id=to, device_id_type=MESH)
        for i, (src, dst, to) in enumerate(
            [(down_half.at[direct:], relay_a, across), (relay_a, relay_b, other)]
        )
    ]
    relay.append(
        pltpu.make_async_remote_copy(
            relay_b, w_down.at[pl.ds(far_down_at + direct, relayed)], r_send.at[2], w_recv.at[last],
            device_id=across, device_id_type=MESH,
        )
    )

    @pl.when(p == 1)
    def _():
        relay[0].start()

    @pl.when(p == 3)
    def _():
        relay[0].wait_recv()
        relay[1].start()
        relay[1].wait_recv()
        relay[2].start()

    @pl.when(lax.rem(p, 2) == 1)
    def _():
        pl.semaphore_wait(turn, 1)

    for copy in far[:last]:
        copy.start()

    @pl.when(p != 1)
    def _():
        far[last].start()

    mixed = n_early + n_dup

    def dups_before(n):
        return jnp.minimum(n, mixed) * n_dup // mixed

    def single_index(n):
        return n - dups_before(n)

    def is_dup(n):
        return dups_before(n + 1) - dups_before(n)

    def row_of(n):
        dup = is_dup(n)
        return dup * (2 * n_single + dups_before(n)) + (1 - dup) * (t * n_single + single_index(n))

    def load(n):
        slot = lax.rem(n, IN_SLOTS)
        return pltpu.make_async_copy(x_hbm.at[row_of(n)], x_in.at[slot], in_sem.at[slot])

    def store(n):
        slot = lax.rem(n, OUT_SLOTS)
        return pltpu.make_async_copy(y_out.at[slot], out_hbm.at[row_of(n)], store_sem.at[slot])

    def hop(n):
        src, dst = lax.rem(n, OUT_SLOTS), lax.rem(n, IN_SLOTS)
        return pltpu.make_async_remote_copy(
            y_out.at[src], x_in.at[dst], hop_sem.at[src], in_sem.at[dst], device_id=after, device_id_type=MESH
        )

    def side(n):
        slot, k = lax.rem(n, OUT_SLOTS), single_index(n)
        return pltpu.make_async_remote_copy(
            y_out.at[slot], out_hbm.at[t * n_single + k], side_send.at[k], side_recv.at[k],
            device_id=other, device_id_type=MESH,
        )

    def keep_late(n):
        slot, k = lax.rem(n, OUT_SLOTS), single_index(n)
        return pltpu.make_async_copy(y_out.at[slot], late_hbm.at[k - n_early], side_send.at[k])

    def send_side(n):
        @pl.when((is_dup(n) == 0) & (single_index(n) < n_early))
        def _():
            side(n).start()

    def reuse(n):
        store(n).wait()

        @pl.when(p < stages - 1)
        def _():
            hop(n).wait_send()

        @pl.when((is_dup(n) == 0) & (single_index(n) < n_early))
        def _():
            side(n).wait_send()

        @pl.when((is_dup(n) == 0) & (single_index(n) >= n_early))
        def _():
            keep_late(n).wait()

    @pl.when(p == 0)
    def _():
        load(0).start()

    def arrived(i):
        near[i].wait()
        far[i].wait_recv()

    for i in range(4):
        arrived(i)
    for c in range(3):
        for m in range(0, width, QUERY_BLOCK):
            w_qkv[:, c * width + m : c * width + m + QUERY_BLOCK] = w_qkv_raw[c, m : m + QUERY_BLOCK, :].T
        for k in range(2):
            for head in range(half_width // head_dim):
                at = c * width + k * half_width + head * head_dim
                b_qkv[:, at : at + head_dim] = b_qkv_raw[k, c, head : head + 1, :].astype(F32)
    for copy in far[:7]:
        copy.wait_send()

    @pl.when(lax.rem(p, 2) == 0)
    def _():
        pl.semaphore_signal(turn, inc=1, device_id=after, device_id_type=MESH)

    for i in range(4, len(far)):
        arrived(i)

    @pl.when(p == 1)
    def _():
        for copy in far[7:last]:
            copy.wait_send()
        pl.semaphore_signal(clear, inc=1, device_id=before, device_id_type=MESH)

    weights = dict(
        g1=g1, c1=c1, qkv=w_qkv, bqkv=b_qkv, out=w_out, bout=bout, g2=g2, c2=c2,
        up=w_up, bup=b_up, down=w_down, bdown=bdown,
    )
    scratch = dict(h=h, qkv=qkv, ctx=ctx, x1=x1, u=u)

    def step(n, carry):
        in_slot, out_slot = lax.rem(n, IN_SLOTS), lax.rem(n, OUT_SLOTS)
        load(n).wait()

        @pl.when((p == 0) & (n + 1 < total))
        def _():
            load(n + 1).start()

        @pl.when(n >= OUT_SLOTS)
        def _():
            reuse(n - OUT_SLOTS)

        one_layer(x_in.at[in_slot], y_out.at[out_slot], weights, scratch, head_dim)

        store(n).start()

        @pl.when((p < stages - 1) & (n >= IN_SLOTS))
        def _():
            pl.semaphore_wait(credit, 1)

        @pl.when(p < stages - 1)
        def _():
            hop(n).start()

        @pl.when((p == 0) & (n == HELD))
        def _():
            pl.semaphore_wait(clear, 1)
            for m in range(HELD):
                send_side(m)

        @pl.when((p != 0) | (n >= HELD))
        def _():
            send_side(n)

        @pl.when((is_dup(n) == 0) & (single_index(n) >= n_early))
        def _():
            keep_late(n).start()

        @pl.when((p > 0) & (n + IN_SLOTS < total))
        def _():
            pl.semaphore_signal(credit, inc=1, device_id=before, device_id_type=MESH)

        return carry

    lax.fori_loop(0, total, step, 0)
    def drain(n, carry):
        reuse(n)
        return carry

    lax.fori_loop(total - OUT_SLOTS, total, drain, 0)

    @pl.when(p != 1)
    def _():
        for copy in far[7:]:
            copy.wait_send()

    @pl.when(p == 1)
    def _():
        relay[0].wait_send()

    @pl.when(p == 3)
    def _():
        relay[1].wait_send()
        relay[2].wait_send()

    def finish(k, carry):
        row = (1 - t) * n_single + k
        pltpu.make_async_copy(out_hbm.at[row], out_hbm.at[row], side_recv.at[k]).wait()
        return carry

    lax.fori_loop(0, n_early, finish, 0)


def copy_kernel(n_single, src, dst, held, sem_in, sem_out):
    slots, count = held.shape[0], src.shape[0]
    begin = (1 - lax.axis_index("tp")) * n_single + n_single
    steps = count - N_LATE

    def row(i):
        return lax.rem(begin + i, count)

    def fetch(i):
        return pltpu.make_async_copy(src.at[row(i)], held.at[i % slots], sem_in.at[i % slots])

    def put(i):
        return pltpu.make_async_copy(held.at[i % slots], dst.at[row(i)], sem_out.at[i % slots])

    ahead = min(slots // 2, steps)
    for i in range(ahead):
        fetch(i).start()
    for i in range(steps):
        if i + ahead < steps:
            if i + ahead >= slots:
                put(i + ahead - slots).wait()
            fetch(i + ahead).start()
        fetch(i).wait()
        put(i).start()
    for i in range(max(steps - slots, 0), steps):
        put(i).wait()


def solution(mesh):
    stages = mesh.shape["pp"]
    weight_specs = (
        P("pp", None), P("pp", None),
        P("pp", None, None, "tp", None), P("pp", None, "tp", None),
        P("pp", "tp", None, None), P("pp", None),
        P("pp", None), P("pp", None),
        P("pp", None, "tp"), P("pp", "tp"),
        P("pp", "tp", None), P("pp", None),
    )

    def local_run(x_micro, g1, c1, w_qkv, b_qkv, w_out, b_out, g2, c2, w_up, b_up, w_down, b_down):
        micro, rows, seq, width = x_micro.shape
        count = micro * rows
        heads, head_dim = w_qkv.shape[3:]
        half_width = heads * head_dim
        half_ff = w_up.shape[2]
        relayed = 2 * half_ff // 3 // 128 * 128
        n_dup = N_DUP
        n_single = (count - n_dup) // 2
        cfg = (stages, n_single, n_dup, head_dim)
        operands = (
            x_micro.reshape(count, seq, width),
            g1, c1, b_out, g2, c2, b_down,
            w_qkv.reshape(3, width, heads, head_dim).transpose(0, 2, 3, 1).reshape(3, half_width, width),
            b_qkv.reshape(3, heads, head_dim),
            w_out.reshape(half_width, width),
            w_up.reshape(width, half_ff),
            b_up.reshape(1, half_ff),
            w_down.reshape(half_ff, width),
        )
        anywhere = pl.BlockSpec(memory_space=pl.ANY)
        vmem = pl.BlockSpec(memory_space=pltpu.VMEM)
        out, late = pl.pallas_call(
            functools.partial(kernel, cfg),
            out_shape=(
                jax.ShapeDtypeStruct((count, seq, width), BF16),
                jax.ShapeDtypeStruct((N_LATE, seq, width), BF16),
            ),
            in_specs=[anywhere] + [vmem] * 6 + [anywhere] * 6,
            out_specs=(anywhere, anywhere),
            scratch_shapes=[
                pltpu.VMEM((3, width, width), BF16),
                pltpu.VMEM((width, 3 * width), BF16),
                pltpu.VMEM((2, 3, heads, head_dim), BF16),
                pltpu.VMEM((1, 3 * width), F32),
                pltpu.VMEM((width, width), BF16),
                pltpu.VMEM((2, width, half_ff), BF16),
                pltpu.VMEM((2, 1, half_ff), BF16),
                pltpu.VMEM((2 * half_ff, width), BF16),
                pltpu.VMEM((relayed, width), BF16),
                pltpu.VMEM((relayed, width), BF16),
                pltpu.VMEM((IN_SLOTS, seq, width), BF16),
                pltpu.VMEM((OUT_SLOTS, seq, width), BF16),
                pltpu.VMEM((seq, width), BF16),
                pltpu.VMEM((seq, 3 * width), BF16),
                pltpu.VMEM((seq, width), BF16),
                pltpu.VMEM((seq, width), BF16),
                pltpu.VMEM((seq, 2 * half_ff), BF16),
                pltpu.SemaphoreType.DMA((9,)),
                pltpu.SemaphoreType.DMA((9,)),
                pltpu.SemaphoreType.DMA((9,)),
                pltpu.SemaphoreType.DMA((3,)),
                pltpu.SemaphoreType.DMA((2,)),
                pltpu.SemaphoreType.DMA((IN_SLOTS,)),
                pltpu.SemaphoreType.DMA((OUT_SLOTS,)),
                pltpu.SemaphoreType.DMA((OUT_SLOTS,)),
                pltpu.SemaphoreType.DMA((n_single,)),
                pltpu.SemaphoreType.DMA((n_single,)),
                pltpu.SemaphoreType.REGULAR,
                pltpu.SemaphoreType.REGULAR,
                pltpu.SemaphoreType.REGULAR,
            ],
            compiler_params=pltpu.CompilerParams(
                collective_id=0,
                has_side_effects=True,
                vmem_limit_bytes=60 * 2**20,
            ),
        )(*operands)
        late = lax.ppermute(late, "tp", [(0, 1), (1, 0)])
        out = pl.pallas_call(
            functools.partial(copy_kernel, n_single),
            out_shape=jax.ShapeDtypeStruct((count, seq, width), BF16),
            in_specs=[anywhere],
            out_specs=anywhere,
            scratch_shapes=[
                pltpu.VMEM((COPY_SLOTS, seq, width), BF16),
                pltpu.SemaphoreType.DMA((COPY_SLOTS,)),
                pltpu.SemaphoreType.DMA((COPY_SLOTS,)),
            ],
            compiler_params=pltpu.CompilerParams(vmem_limit_bytes=60 * 2**20),
            cost_estimate=pl.CostEstimate(
                flops=5 * 10**10, transcendentals=0, bytes_accessed=4 * count * seq * width
            ),
        )(out)
        first = (1 - lax.axis_index("tp")) * n_single + n_single - N_LATE
        out = lax.dynamic_update_slice(out, late, (first, 0, 0))
        return out.reshape(1, micro, rows, seq, width)

    return jax.shard_map(
        local_run,
        mesh=mesh,
        in_specs=(P(None, "dp", None, None),) + weight_specs,
        out_specs=P("pp", None, "dp", None, None),
        check_vma=False,
    )
```

```python
import functools
import math

import jax
import jax.numpy as jnp
from jax import lax
from jax.experimental import pallas as pl
from jax.experimental.pallas import tpu as pltpu
from jax.sharding import PartitionSpec as P

F32 = jnp.float32
BF16 = jnp.bfloat16
MESH = pl.DeviceIdType.MESH
LN_EPS = 1e-5
N_DUP = 16
N_LATE = 3
IN_SLOTS = 4
OUT_SLOTS = 8
HELD = 2
QUERY_BLOCK = 256
COL_BLOCK = 768
ROW_BLOCK = 128
MID_ROW_BLOCK = 256
COPY_SLOTS = 48
GELU_C0 = math.sqrt(2.0 / math.pi)
GELU_C1 = GELU_C0 * 0.044715


def dot(a, b, ca=1, cb=0):
    return lax.dot_general(a, b, (((ca,), (cb,)), ((), ())), preferred_element_type=F32)


def layer_norm(x, gain, bias):
    x = x.astype(F32)
    mean = jnp.mean(x, axis=-1, keepdims=True)
    centered = x - mean
    var = jnp.mean(centered * centered, axis=-1, keepdims=True)
    return (centered * lax.rsqrt(var + LN_EPS) * gain.astype(F32) + bias.astype(F32)).astype(BF16)


def gelu(z):
    return z * jax.nn.sigmoid(z * (2.0 * GELU_C0 + 2.0 * GELU_C1 * (z * z)))


def attention(qkv, ctx, head_dim):
    seq, width = ctx.shape
    pair = 2 * head_dim
    scale = head_dim**-0.5 * math.log2(math.e)
    first = lax.broadcasted_iota(jnp.int32, (1, pair), 1) < head_dim
    zero = jnp.zeros((), BF16)
    block = QUERY_BLOCK
    keep = lax.broadcasted_iota(jnp.int32, (block, block), 0) >= lax.broadcasted_iota(jnp.int32, (block, block), 1)
    keep = jnp.concatenate([keep, keep], axis=0)
    for q0 in range(seq - block, -1, -block):
        for p in range(width // pair):
            lanes = slice(p * pair, (p + 1) * pair)
            keys = qkv[: q0 + block, width + p * pair : width + (p + 1) * pair]
            values = qkv[: q0 + block, 2 * width + p * pair : 2 * width + (p + 1) * pair]
            q = qkv[q0 : q0 + block, lanes]
            q = jnp.concatenate([jnp.where(first, q, zero), jnp.where(first, zero, q)], axis=0)
            scores = dot(q, keys, 1, 1)
            diag = jnp.where(keep, scores[:, q0:], -1e30)
            scores = jnp.concatenate([scores[:, :q0], diag], axis=1) if q0 else diag
            top = jnp.max(scores, axis=-1, keepdims=True)
            probs = jnp.exp2((scores - top) * scale)
            total = jnp.sum(probs, axis=-1, keepdims=True)
            out = dot(probs.astype(BF16), values) * (1.0 / total)
            ctx[q0 : q0 + block, lanes] = jnp.where(first, out[:block], out[block:]).astype(BF16)


def col_blocks(size):
    block = min(COL_BLOCK, size)
    return [slice(n, n + block) for n in range(0, size, block)]


def project_residual(lhs, weight, bias, resid, out, rows, cols):
    part = (dot(lhs[rows], weight[:, cols]) + bias[:, cols].astype(F32)).astype(BF16)
    out[rows, cols] = (resid[rows, cols].astype(F32) + part.astype(F32)).astype(BF16)


def one_layer(x, y, w, s, head_dim):
    seq, width = x.shape
    blocks = [slice(m, m + ROW_BLOCK) for m in range(0, seq, ROW_BLOCK)]
    for rows in blocks:
        s["h"][rows] = layer_norm(x[rows], w["g1"][...], w["c1"][...])
        for cols in col_blocks(3 * width):
            s["qkv"][rows, cols] = (dot(s["h"][rows], w["qkv"][:, cols]) + w["bqkv"][:, cols]).astype(BF16)
    attention(s["qkv"], s["ctx"], head_dim)
    for m in range(0, seq, MID_ROW_BLOCK):
        rows = slice(m, m + MID_ROW_BLOCK)
        for cols in col_blocks(width):
            project_residual(s["ctx"], w["out"], w["bout"], x, s["x1"], rows, cols)
        s["h"][rows] = layer_norm(s["x1"][rows], w["g2"][...], w["c2"][...])
    half = w["up"].shape[2]
    for t in range(2):
        for cols in col_blocks(half):
            for rows in blocks:
                z = dot(s["h"][rows], w["up"][t, :, cols]) + w["bup"][t, :, cols].astype(F32)
                s["u"][rows, t * half + cols.start : t * half + cols.stop] = gelu(z).astype(BF16)
    for cols in col_blocks(width):
        for rows in blocks:
            project_residual(s["u"], w["down"], w["bdown"], s["x1"], y, rows, cols)


def kernel(
    cfg,
    x_hbm, g1, c1, bout, g2, c2, bdown, qkv_half, bqkv_half, out_half, up_half, bup_half, down_half,
    out_hbm, late_hbm,
    w_qkv_raw, w_qkv, b_qkv_raw, b_qkv, w_out, w_up, b_up, w_down,
    relay_a, relay_b, x_in, y_out, h, qkv, ctx, x1, u,
    w_local, w_send, w_recv, r_send, r_recv, in_sem, store_sem, hop_sem, side_send, side_recv, credit, turn, clear,
):
    stages, n_single, n_dup, head_dim = cfg
    n_early = n_single - late_hbm.shape[0]
    total = n_single + n_dup
    t = lax.axis_index("tp")
    p = lax.axis_index("pp")
    width = x_hbm.shape[2]
    half_width = width // 2
    other = {"tp": 1 - t}
    after = {"pp": lax.rem(p + 1, stages)}
    before = {"pp": lax.rem(p + stages - 1, stages)}

    across = {"pp": lax.rem(p + 2, stages)}

    barrier = pltpu.get_barrier_semaphore()
    for peer in (other, after, before, across):
        pl.semaphore_signal(barrier, inc=1, device_id=peer, device_id_type=MESH)
    pl.semaphore_wait(barrier, 4)

    half_ff = down_half.shape[0]
    mine = pl.ds(pl.multiple_of(t * half_width, 128), half_width)
    pieces = [(qkv_half.at[c], w_qkv_raw.at[c, mine]) for c in range(3)]
    pieces.append((bqkv_half, b_qkv_raw.at[t]))
    pieces.append((out_half, w_out.at[mine]))
    pieces.append((bup_half, b_up.at[t]))
    pieces.append((up_half, w_up.at[t]))
    relayed = relay_a.shape[0]
    direct = half_ff - relayed
    down_at = pl.multiple_of(t * half_ff, 128)
    pieces.append((down_half.at[:direct], w_down.at[pl.ds(down_at, direct)]))
    pieces.append((down_half.at[direct:], w_down.at[pl.ds(down_at + direct, relayed)]))
    near, far = [], []
    for i, (src, dst) in enumerate(pieces):
        near.append(pltpu.make_async_copy(src, dst, w_local.at[i]))
        far.append(
            pltpu.make_async_remote_copy(src, dst, w_send.at[i], w_recv.at[i], device_id=other, device_id_type=MESH)
        )
        near[-1].start()

    last = len(pieces) - 1
    far_down_at = pl.multiple_of((1 - t) * half_ff, 128)
    relay = [
        pltpu.make_async_remote_copy(src, dst, r_send.at[i], r_recv.at[i], device_id=to, device_id_type=MESH)
        for i, (src, dst, to) in enumerate(
            [(down_half.at[direct:], relay_a, across), (relay_a, relay_b, other)]
        )
    ]
    relay.append(
        pltpu.make_async_remote_copy(
            relay_b, w_down.at[pl.ds(far_down_at + direct, relayed)], r_send.at[2], w_recv.at[last],
            device_id=across, device_id_type=MESH,
        )
    )

    @pl.when(p == 1)
    def _():
        relay[0].start()

    @pl.when(p == 3)
    def _():
        relay[0].wait_recv()
        relay[1].start()
        relay[1].wait_recv()
        relay[2].start()

    @pl.when(lax.rem(p, 2) == 1)
    def _():
        pl.semaphore_wait(turn, 1)

    for copy in far[:last]:
        copy.start()

    @pl.when(p != 1)
    def _():
        far[last].start()

    mixed = n_early + n_dup

    share = -(-512 * n_dup // mixed)
    assert [m * share // 512 for m in (0, mixed)] == [0, n_dup]

    def dups_before(n):
        return lax.div(jnp.minimum(n, mixed) * share, 512)

    def single_index(n):
        return n - dups_before(n)

    def is_dup(n):
        return dups_before(n + 1) - dups_before(n)

    def row_of(n):
        dup = is_dup(n)
        return dup * (2 * n_single + dups_before(n)) + (1 - dup) * (t * n_single + single_index(n))

    def load(n):
        slot = lax.rem(n, IN_SLOTS)
        return pltpu.make_async_copy(x_hbm.at[row_of(n)], x_in.at[slot], in_sem.at[slot])

    def store(n):
        slot = lax.rem(n, OUT_SLOTS)
        return pltpu.make_async_copy(y_out.at[slot], out_hbm.at[row_of(n)], store_sem.at[slot])

    def hop(n):
        src, dst = lax.rem(n, OUT_SLOTS), lax.rem(n, IN_SLOTS)
        return pltpu.make_async_remote_copy(
            y_out.at[src], x_in.at[dst], hop_sem.at[src], in_sem.at[dst], device_id=after, device_id_type=MESH
        )

    def side(n):
        slot, k = lax.rem(n, OUT_SLOTS), single_index(n)
        return pltpu.make_async_remote_copy(
            y_out.at[slot], out_hbm.at[t * n_single + k], side_send.at[k], side_recv.at[k],
            device_id=other, device_id_type=MESH,
        )

    def keep_late(n):
        slot, k = lax.rem(n, OUT_SLOTS), single_index(n)
        return pltpu.make_async_copy(y_out.at[slot], late_hbm.at[k - n_early], side_send.at[k])

    def send_side(n):
        @pl.when((is_dup(n) == 0) & (single_index(n) < n_early))
        def _():
            side(n).start()

    def reuse(n):
        store(n).wait()

        @pl.when(p < stages - 1)
        def _():
            hop(n).wait_send()

        @pl.when((is_dup(n) == 0) & (single_index(n) < n_early))
        def _():
            side(n).wait_send()

        @pl.when((is_dup(n) == 0) & (single_index(n) >= n_early))
        def _():
            keep_late(n).wait()

    @pl.when(p == 0)
    def _():
        load(0).start()

    def arrived(i):
        near[i].wait()
        far[i].wait_recv()

    for i in range(4):
        arrived(i)
    for c in range(3):
        for m in range(0, width, QUERY_BLOCK):
            w_qkv[:, c * width + m : c * width + m + QUERY_BLOCK] = w_qkv_raw[c, m : m + QUERY_BLOCK, :].T
        for k in range(2):
            for head in range(half_width // head_dim):
                at = c * width + k * half_width + head * head_dim
                b_qkv[:, at : at + head_dim] = b_qkv_raw[k, c, head : head + 1, :].astype(F32)
    for copy in far[:7]:
        copy.wait_send()

    @pl.when(lax.rem(p, 2) == 0)
    def _():
        pl.semaphore_signal(turn, inc=1, device_id=after, device_id_type=MESH)

    for i in range(4, len(far)):
        arrived(i)

    @pl.when(p == 1)
    def _():
        for copy in far[7:last]:
            copy.wait_send()
        pl.semaphore_signal(clear, inc=1, device_id=before, device_id_type=MESH)

    weights = dict(
        g1=g1, c1=c1, qkv=w_qkv, bqkv=b_qkv, out=w_out, bout=bout, g2=g2, c2=c2,
        up=w_up, bup=b_up, down=w_down, bdown=bdown,
    )
    scratch = dict(h=h, qkv=qkv, ctx=ctx, x1=x1, u=u)

    def step(n, carry):
        in_slot, out_slot = lax.rem(n, IN_SLOTS), lax.rem(n, OUT_SLOTS)
        load(n).wait()

        @pl.when((p == 0) & (n + 1 < total))
        def _():
            load(n + 1).start()

        @pl.when(n >= OUT_SLOTS)
        def _():
            reuse(n - OUT_SLOTS)

        one_layer(x_in.at[in_slot], y_out.at[out_slot], weights, scratch, head_dim)

        store(n).start()

        @pl.when((p < stages - 1) & (n >= IN_SLOTS))
        def _():
            pl.semaphore_wait(credit, 1)

        @pl.when(p < stages - 1)
        def _():
            hop(n).start()

        @pl.when((p == 0) & (n == HELD))
        def _():
            pl.semaphore_wait(clear, 1)
            for m in range(HELD):
                send_side(m)

        @pl.when((p != 0) | (n >= HELD))
        def _():
            send_side(n)

        @pl.when((is_dup(n) == 0) & (single_index(n) >= n_early))
        def _():
            keep_late(n).start()

        @pl.when((p > 0) & (n + IN_SLOTS < total))
        def _():
            pl.semaphore_signal(credit, inc=1, device_id=before, device_id_type=MESH)

        return carry

    lax.fori_loop(0, total, step, 0)
    def drain(n, carry):
        reuse(n)
        return carry

    lax.fori_loop(total - OUT_SLOTS, total, drain, 0)

    @pl.when(p != 1)
    def _():
        for copy in far[7:]:
            copy.wait_send()

    @pl.when(p == 1)
    def _():
        relay[0].wait_send()

    @pl.when(p == 3)
    def _():
        relay[1].wait_send()
        relay[2].wait_send()

    def finish(k, carry):
        row = (1 - t) * n_single + k
        pltpu.make_async_copy(out_hbm.at[row], out_hbm.at[row], side_recv.at[k]).wait()
        return carry

    lax.fori_loop(0, n_early, finish, 0)


def copy_kernel(n_single, src, dst, held, sem_in, sem_out):
    slots, count = held.shape[0], src.shape[0]
    begin = (1 - lax.axis_index("tp")) * n_single + n_single
    steps = count - N_LATE

    def row(i):
        return lax.rem(begin + i, count)

    def fetch(i):
        return pltpu.make_async_copy(src.at[row(i)], held.at[i % slots], sem_in.at[i % slots])

    def put(i):
        return pltpu.make_async_copy(held.at[i % slots], dst.at[row(i)], sem_out.at[i % slots])

    ahead = min(slots // 2, steps)
    for i in range(ahead):
        fetch(i).start()
    for i in range(steps):
        if i + ahead < steps:
            if i + ahead >= slots:
                put(i + ahead - slots).wait()
            fetch(i + ahead).start()
        fetch(i).wait()
        put(i).start()
    for i in range(max(steps - slots, 0), steps):
        put(i).wait()


def solution(mesh):
    stages = mesh.shape["pp"]
    weight_specs = (
        P("pp", None), P("pp", None),
        P("pp", None, None, "tp", None), P("pp", None, "tp", None),
        P("pp", "tp", None, None), P("pp", None),
        P("pp", None), P("pp", None),
        P("pp", None, "tp"), P("pp", "tp"),
        P("pp", "tp", None), P("pp", None),
    )

    def local_run(x_micro, g1, c1, w_qkv, b_qkv, w_out, b_out, g2, c2, w_up, b_up, w_down, b_down):
        micro, rows, seq, width = x_micro.shape
        count = micro * rows
        heads, head_dim = w_qkv.shape[3:]
        half_width = heads * head_dim
        half_ff = w_up.shape[2]
        relayed = 2 * half_ff // 3 // 128 * 128
        n_dup = N_DUP
        n_single = (count - n_dup) // 2
        cfg = (stages, n_single, n_dup, head_dim)
        operands = (
            x_micro.reshape(count, seq, width),
            g1, c1, b_out, g2, c2, b_down,
            w_qkv.reshape(3, width, heads, head_dim).transpose(0, 2, 3, 1).reshape(3, half_width, width),
            b_qkv.reshape(3, heads, head_dim),
            w_out.reshape(half_width, width),
            w_up.reshape(width, half_ff),
            b_up.reshape(1, half_ff),
            w_down.reshape(half_ff, width),
        )
        anywhere = pl.BlockSpec(memory_space=pl.ANY)
        vmem = pl.BlockSpec(memory_space=pltpu.VMEM)
        out, late = pl.pallas_call(
            functools.partial(kernel, cfg),
            out_shape=(
                jax.ShapeDtypeStruct((count, seq, width), BF16),
                jax.ShapeDtypeStruct((N_LATE, seq, width), BF16),
            ),
            in_specs=[anywhere] + [vmem] * 6 + [anywhere] * 6,
            out_specs=(anywhere, anywhere),
            scratch_shapes=[
                pltpu.VMEM((3, width, width), BF16),
                pltpu.VMEM((width, 3 * width), BF16),
                pltpu.VMEM((2, 3, heads, head_dim), BF16),
                pltpu.VMEM((1, 3 * width), F32),
                pltpu.VMEM((width, width), BF16),
                pltpu.VMEM((2, width, half_ff), BF16),
                pltpu.VMEM((2, 1, half_ff), BF16),
                pltpu.VMEM((2 * half_ff, width), BF16),
                pltpu.VMEM((relayed, width), BF16),
                pltpu.VMEM((relayed, width), BF16),
                pltpu.VMEM((IN_SLOTS, seq, width), BF16),
                pltpu.VMEM((OUT_SLOTS, seq, width), BF16),
                pltpu.VMEM((seq, width), BF16),
                pltpu.VMEM((seq, 3 * width), BF16),
                pltpu.VMEM((seq, width), BF16),
                pltpu.VMEM((seq, width), BF16),
                pltpu.VMEM((seq, 2 * half_ff), BF16),
                pltpu.SemaphoreType.DMA((9,)),
                pltpu.SemaphoreType.DMA((9,)),
                pltpu.SemaphoreType.DMA((9,)),
                pltpu.SemaphoreType.DMA((3,)),
                pltpu.SemaphoreType.DMA((2,)),
                pltpu.SemaphoreType.DMA((IN_SLOTS,)),
                pltpu.SemaphoreType.DMA((OUT_SLOTS,)),
                pltpu.SemaphoreType.DMA((OUT_SLOTS,)),
                pltpu.SemaphoreType.DMA((n_single,)),
                pltpu.SemaphoreType.DMA((n_single,)),
                pltpu.SemaphoreType.REGULAR,
                pltpu.SemaphoreType.REGULAR,
                pltpu.SemaphoreType.REGULAR,
            ],
            compiler_params=pltpu.CompilerParams(
                collective_id=0,
                has_side_effects=True,
                vmem_limit_bytes=60 * 2**20,
            ),
        )(*operands)
        late = lax.ppermute(late, "tp", [(0, 1), (1, 0)])
        out = pl.pallas_call(
            functools.partial(copy_kernel, n_single),
            out_shape=jax.ShapeDtypeStruct((count, seq, width), BF16),
            in_specs=[anywhere],
            out_specs=anywhere,
            scratch_shapes=[
                pltpu.VMEM((COPY_SLOTS, seq, width), BF16),
                pltpu.SemaphoreType.DMA((COPY_SLOTS,)),
                pltpu.SemaphoreType.DMA((COPY_SLOTS,)),
            ],
            compiler_params=pltpu.CompilerParams(vmem_limit_bytes=60 * 2**20),
            cost_estimate=pl.CostEstimate(
                flops=5 * 10**10, transcendentals=0, bytes_accessed=4 * count * seq * width
            ),
        )(out)
        first = (1 - lax.axis_index("tp")) * n_single + n_single - N_LATE
        out = lax.dynamic_update_slice(out, late, (first, 0, 0))
        return out.reshape(1, micro, rows, seq, width)

    return jax.shard_map(
        local_run,
        mesh=mesh,
        in_specs=(P(None, "dp", None, None),) + weight_specs,
        out_specs=P("pp", None, "dp", None, None),
        check_vma=False,
    )
```

```python
import functools
import math

import jax
import jax.numpy as jnp
from jax import lax
from jax.experimental import pallas as pl
from jax.experimental.pallas import tpu as pltpu
from jax.sharding import PartitionSpec as P

F32 = jnp.float32
BF16 = jnp.bfloat16
MESH = pl.DeviceIdType.MESH
LN_EPS = 1e-5
N_DUP = 16
N_LATE = 3
IN_SLOTS = 4
OUT_SLOTS = 8
HELD = 2
QUERY_BLOCK = 256
COL_BLOCK = 768
ROW_BLOCK = 128
MID_ROW_BLOCK = 256
COPY_SLOTS = 48
GELU_C0 = math.sqrt(2.0 / math.pi)
GELU_C1 = GELU_C0 * 0.044715


def dot(a, b, ca=1, cb=0):
    return lax.dot_general(a, b, (((ca,), (cb,)), ((), ())), preferred_element_type=F32)


def layer_norm(x, gain, bias):
    x = x.astype(F32)
    mean = jnp.mean(x, axis=-1, keepdims=True)
    centered = x - mean
    var = jnp.mean(centered * centered, axis=-1, keepdims=True)
    return (centered * lax.rsqrt(var + LN_EPS) * gain.astype(F32) + bias.astype(F32)).astype(BF16)


def gelu(z):
    return z * jax.nn.sigmoid(z * (2.0 * GELU_C0 + 2.0 * GELU_C1 * (z * z)))


def attention(qkv, ctx, head_dim):
    seq, width = ctx.shape
    pair = 2 * head_dim
    scale = head_dim**-0.5 * math.log2(math.e)
    first = lax.broadcasted_iota(jnp.int32, (1, pair), 1) < head_dim
    zero = jnp.zeros((), BF16)
    block = QUERY_BLOCK
    quarter = block // 2
    keep = lax.broadcasted_iota(jnp.int32, (quarter, quarter), 0) >= lax.broadcasted_iota(
        jnp.int32, (quarter, quarter), 1
    )
    hidden = jnp.full((quarter, quarter), -1e30, F32)
    for q0 in range(seq - block, -1, -block):
        for p in range(width // pair):
            lanes = slice(p * pair, (p + 1) * pair)
            keys = qkv[: q0 + block, width + p * pair : width + (p + 1) * pair]
            values = qkv[: q0 + block, 2 * width + p * pair : 2 * width + (p + 1) * pair]
            q = qkv[q0 : q0 + block, lanes]
            q = jnp.concatenate([jnp.where(first, q, zero), jnp.where(first, zero, q)], axis=0)
            scores = dot(q, keys, 1, 1)
            split, end = q0 + quarter, q0 + block
            rows = []
            for m in (0, block):
                upper = jnp.where(keep, scores[m : m + quarter, q0:split], -1e30)
                lower = jnp.where(keep, scores[m + quarter : m + block, split:end], -1e30)
                rows.append(jnp.concatenate([upper, hidden], axis=1))
                rows.append(jnp.concatenate([scores[m + quarter : m + block, q0:split], lower], axis=1))
            diag = jnp.concatenate(rows, axis=0)
            scores = jnp.concatenate([scores[:, :q0], diag], axis=1) if q0 else diag
            top = jnp.max(scores, axis=-1, keepdims=True)
            probs = jnp.exp2((scores - top) * scale)
            rows = []
            for m in (0, block):
                rows.append(jnp.concatenate([probs[m : m + quarter, :split], jnp.zeros_like(hidden)], axis=1))
                rows.append(probs[m + quarter : m + block])
            probs = jnp.concatenate(rows, axis=0)
            total = jnp.sum(probs, axis=-1, keepdims=True)
            out = dot(probs.astype(BF16), values) * (1.0 / total)
            ctx[q0 : q0 + block, lanes] = jnp.where(first, out[:block], out[block:]).astype(BF16)


def col_blocks(size):
    block = min(COL_BLOCK, size)
    return [slice(n, n + block) for n in range(0, size, block)]


def project_residual(lhs, weight, bias, resid, out, rows, cols):
    part = (dot(lhs[rows], weight[:, cols]) + bias[:, cols].astype(F32)).astype(BF16)
    out[rows, cols] = (resid[rows, cols].astype(F32) + part.astype(F32)).astype(BF16)


def one_layer(x, y, w, s, head_dim):
    seq, width = x.shape
    blocks = [slice(m, m + ROW_BLOCK) for m in range(0, seq, ROW_BLOCK)]
    for rows in blocks:
        s["h"][rows] = layer_norm(x[rows], w["g1"][...], w["c1"][...])
        for cols in col_blocks(3 * width):
            s["qkv"][rows, cols] = (dot(s["h"][rows], w["qkv"][:, cols]) + w["bqkv"][:, cols]).astype(BF16)
    attention(s["qkv"], s["ctx"], head_dim)
    for m in range(seq - MID_ROW_BLOCK, -1, -MID_ROW_BLOCK):
        rows = slice(m, m + MID_ROW_BLOCK)
        for cols in col_blocks(width):
            project_residual(s["ctx"], w["out"], w["bout"], x, s["x1"], rows, cols)
        s["h"][rows] = layer_norm(s["x1"][rows], w["g2"][...], w["c2"][...])
    half = w["up"].shape[2]
    blocks = blocks[len(blocks) // 2 :] + blocks[: len(blocks) // 2]
    for t in range(2):
        for cols in col_blocks(half):
            for rows in blocks:
                z = dot(s["h"][rows], w["up"][t, :, cols]) + w["bup"][t, :, cols].astype(F32)
                s["u"][rows, t * half + cols.start : t * half + cols.stop] = gelu(z).astype(BF16)
    for cols in col_blocks(width):
        for rows in blocks:
            project_residual(s["u"], w["down"], w["bdown"], s["x1"], y, rows, cols)


def kernel(
    cfg,
    x_hbm, g1, c1, bout, g2, c2, bdown, qkv_half, bqkv_half, out_half, up_half, bup_half, down_half,
    out_hbm, late_hbm,
    w_qkv_raw, w_qkv, b_qkv_raw, b_qkv, w_out, w_up, b_up, w_down,
    relay_a, relay_b, x_in, y_out, h, qkv, ctx, x1, u,
    w_local, w_send, w_recv, r_send, r_recv, in_sem, store_sem, hop_sem, side_send, side_recv, credit, turn, clear,
):
    stages, n_single, n_dup, head_dim = cfg
    n_early = n_single - late_hbm.shape[0]
    total = n_single + n_dup
    t = lax.axis_index("tp")
    p = lax.axis_index("pp")
    width = x_hbm.shape[2]
    half_width = width // 2
    other = {"tp": 1 - t}
    after = {"pp": lax.rem(p + 1, stages)}
    before = {"pp": lax.rem(p + stages - 1, stages)}

    across = {"pp": lax.rem(p + 2, stages)}

    barrier = pltpu.get_barrier_semaphore()
    for peer in (other, after, before, across):
        pl.semaphore_signal(barrier, inc=1, device_id=peer, device_id_type=MESH)
    pl.semaphore_wait(barrier, 4)

    half_ff = down_half.shape[0]
    mine = pl.ds(pl.multiple_of(t * half_width, 128), half_width)
    pieces = [(qkv_half.at[c], w_qkv_raw.at[c, mine]) for c in range(3)]
    pieces.append((bqkv_half, b_qkv_raw.at[t]))
    pieces.append((out_half, w_out.at[mine]))
    pieces.append((bup_half, b_up.at[t]))
    pieces.append((up_half, w_up.at[t]))
    relayed = relay_a.shape[0]
    direct = half_ff - relayed
    down_at = pl.multiple_of(t * half_ff, 128)
    pieces.append((down_half.at[:direct], w_down.at[pl.ds(down_at, direct)]))
    pieces.append((down_half.at[direct:], w_down.at[pl.ds(down_at + direct, relayed)]))
    near, far = [], []
    for i, (src, dst) in enumerate(pieces):
        near.append(pltpu.make_async_copy(src, dst, w_local.at[i]))
        far.append(
            pltpu.make_async_remote_copy(src, dst, w_send.at[i], w_recv.at[i], device_id=other, device_id_type=MESH)
        )
        near[-1].start()

    last = len(pieces) - 1
    far_down_at = pl.multiple_of((1 - t) * half_ff, 128)
    relay = [
        pltpu.make_async_remote_copy(src, dst, r_send.at[i], r_recv.at[i], device_id=to, device_id_type=MESH)
        for i, (src, dst, to) in enumerate(
            [(down_half.at[direct:], relay_a, across), (relay_a, relay_b, other)]
        )
    ]
    relay.append(
        pltpu.make_async_remote_copy(
            relay_b, w_down.at[pl.ds(far_down_at + direct, relayed)], r_send.at[2], w_recv.at[last],
            device_id=across, device_id_type=MESH,
        )
    )

    @pl.when(p == 1)
    def _():
        relay[0].start()

    @pl.when(p == 3)
    def _():
        relay[0].wait_recv()
        relay[1].start()
        relay[1].wait_recv()
        relay[2].start()

    @pl.when(lax.rem(p, 2) == 1)
    def _():
        pl.semaphore_wait(turn, 1)

    for copy in far[:last]:
        copy.start()

    @pl.when(p != 1)
    def _():
        far[last].start()

    mixed = n_early + n_dup

    share = -(-512 * n_dup // mixed)
    assert [m * share // 512 for m in (0, mixed)] == [0, n_dup]

    def dups_before(n):
        return lax.div(jnp.minimum(n, mixed) * share, 512)

    def single_index(n):
        return n - dups_before(n)

    def is_dup(n):
        return dups_before(n + 1) - dups_before(n)

    def row_of(n):
        dup = is_dup(n)
        return dup * (2 * n_single + dups_before(n)) + (1 - dup) * (t * n_single + single_index(n))

    def load(n):
        slot = lax.rem(n, IN_SLOTS)
        return pltpu.make_async_copy(x_hbm.at[row_of(n)], x_in.at[slot], in_sem.at[slot])

    def store(n):
        slot = lax.rem(n, OUT_SLOTS)
        return pltpu.make_async_copy(y_out.at[slot], out_hbm.at[row_of(n)], store_sem.at[slot])

    def hop(n):
        src, dst = lax.rem(n, OUT_SLOTS), lax.rem(n, IN_SLOTS)
        return pltpu.make_async_remote_copy(
            y_out.at[src], x_in.at[dst], hop_sem.at[src], in_sem.at[dst], device_id=after, device_id_type=MESH
        )

    def side(n):
        slot, k = lax.rem(n, OUT_SLOTS), single_index(n)
        return pltpu.make_async_remote_copy(
            y_out.at[slot], out_hbm.at[t * n_single + k], side_send.at[k], side_recv.at[k],
            device_id=other, device_id_type=MESH,
        )

    def keep_late(n):
        slot, k = lax.rem(n, OUT_SLOTS), single_index(n)
        return pltpu.make_async_copy(y_out.at[slot], late_hbm.at[k - n_early], side_send.at[k])

    def send_side(n):
        @pl.when((is_dup(n) == 0) & (single_index(n) < n_early))
        def _():
            side(n).start()

    def reuse(n):
        store(n).wait()

        @pl.when(p < stages - 1)
        def _():
            hop(n).wait_send()

        @pl.when((is_dup(n) == 0) & (single_index(n) < n_early))
        def _():
            side(n).wait_send()

        @pl.when((is_dup(n) == 0) & (single_index(n) >= n_early))
        def _():
            keep_late(n).wait()

    @pl.when(p == 0)
    def _():
        load(0).start()

    def arrived(i):
        near[i].wait()
        far[i].wait_recv()

    for i in range(4):
        arrived(i)
    for c in range(3):
        for m in range(0, width, QUERY_BLOCK):
            w_qkv[:, c * width + m : c * width + m + QUERY_BLOCK] = w_qkv_raw[c, m : m + QUERY_BLOCK, :].T
        for k in range(2):
            for head in range(half_width // head_dim):
                at = c * width + k * half_width + head * head_dim
                b_qkv[:, at : at + head_dim] = b_qkv_raw[k, c, head : head + 1, :].astype(F32)
    @pl.when(lax.rem(p, 2) == 0)
    def _():
        for copy in far[:7]:
            copy.wait_send()
        pl.semaphore_signal(turn, inc=1, device_id=after, device_id_type=MESH)

    for i in range(4, len(far)):
        arrived(i)

    @pl.when(p == 1)
    def _():
        for copy in far[:last]:
            copy.wait_send()
        pl.semaphore_signal(clear, inc=1, device_id=before, device_id_type=MESH)

    weights = dict(
        g1=g1, c1=c1, qkv=w_qkv, bqkv=b_qkv, out=w_out, bout=bout, g2=g2, c2=c2,
        up=w_up, bup=b_up, down=w_down, bdown=bdown,
    )
    scratch = dict(h=h, qkv=qkv, ctx=ctx, x1=x1, u=u)

    def step(n, carry):
        in_slot, out_slot = lax.rem(n, IN_SLOTS), lax.rem(n, OUT_SLOTS)
        load(n).wait()

        @pl.when((p == 0) & (n + 1 < total))
        def _():
            load(n + 1).start()

        @pl.when(n >= OUT_SLOTS)
        def _():
            reuse(n - OUT_SLOTS)

        one_layer(x_in.at[in_slot], y_out.at[out_slot], weights, scratch, head_dim)

        store(n).start()

        @pl.when((p < stages - 1) & (n >= IN_SLOTS))
        def _():
            pl.semaphore_wait(credit, 1)

        @pl.when(p < stages - 1)
        def _():
            hop(n).start()

        @pl.when((p == 0) & (n == HELD))
        def _():
            pl.semaphore_wait(clear, 1)
            for m in range(HELD):
                send_side(m)

        @pl.when((p != 0) | (n >= HELD))
        def _():
            send_side(n)

        @pl.when((is_dup(n) == 0) & (single_index(n) >= n_early))
        def _():
            keep_late(n).start()

        @pl.when((p > 0) & (n + IN_SLOTS < total))
        def _():
            pl.semaphore_signal(credit, inc=1, device_id=before, device_id_type=MESH)

        return carry

    lax.fori_loop(0, total, step, 0)
    def drain(n, carry):
        reuse(n)
        return carry

    lax.fori_loop(total - OUT_SLOTS, total, drain, 0)

    @pl.when(lax.rem(p, 2) == 0)
    def _():
        for copy in far[7:]:
            copy.wait_send()

    @pl.when(p == 3)
    def _():
        for copy in far:
            copy.wait_send()

    @pl.when(p == 1)
    def _():
        relay[0].wait_send()

    @pl.when(p == 3)
    def _():
        relay[1].wait_send()
        relay[2].wait_send()

    def finish(k, carry):
        row = (1 - t) * n_single + k
        pltpu.make_async_copy(out_hbm.at[row], out_hbm.at[row], side_recv.at[k]).wait()
        return carry

    lax.fori_loop(0, n_early, finish, 0)


def copy_kernel(n_single, src, dst, held, sem_in, sem_out):
    slots, count = held.shape[0], src.shape[0]
    begin = (1 - lax.axis_index("tp")) * n_single + n_single
    steps = count - N_LATE

    def row(i):
        return lax.rem(begin + i, count)

    def fetch(i):
        return pltpu.make_async_copy(src.at[row(i)], held.at[i % slots], sem_in.at[i % slots])

    def put(i):
        return pltpu.make_async_copy(held.at[i % slots], dst.at[row(i)], sem_out.at[i % slots])

    ahead = min(slots // 2, steps)
    for i in range(ahead):
        fetch(i).start()
    for i in range(steps):
        if i + ahead < steps:
            if i + ahead >= slots:
                put(i + ahead - slots).wait()
            fetch(i + ahead).start()
        fetch(i).wait()
        put(i).start()
    for i in range(max(steps - slots, 0), steps):
        put(i).wait()


def solution(mesh):
    stages = mesh.shape["pp"]
    weight_specs = (
        P("pp", None), P("pp", None),
        P("pp", None, None, "tp", None), P("pp", None, "tp", None),
        P("pp", "tp", None, None), P("pp", None),
        P("pp", None), P("pp", None),
        P("pp", None, "tp"), P("pp", "tp"),
        P("pp", "tp", None), P("pp", None),
    )

    def local_run(x_micro, g1, c1, w_qkv, b_qkv, w_out, b_out, g2, c2, w_up, b_up, w_down, b_down):
        micro, rows, seq, width = x_micro.shape
        count = micro * rows
        heads, head_dim = w_qkv.shape[3:]
        half_width = heads * head_dim
        half_ff = w_up.shape[2]
        relayed = 2 * half_ff // 3 // 128 * 128
        n_dup = N_DUP
        n_single = (count - n_dup) // 2
        cfg = (stages, n_single, n_dup, head_dim)
        operands = (
            x_micro.reshape(count, seq, width),
            g1, c1, b_out, g2, c2, b_down,
            w_qkv.reshape(3, width, heads, head_dim).transpose(0, 2, 3, 1).reshape(3, half_width, width),
            b_qkv.reshape(3, heads, head_dim),
            w_out.reshape(half_width, width),
            w_up.reshape(width, half_ff),
            b_up.reshape(1, half_ff),
            w_down.reshape(half_ff, width),
        )
        anywhere = pl.BlockSpec(memory_space=pl.ANY)
        vmem = pl.BlockSpec(memory_space=pltpu.VMEM)
        out, late = pl.pallas_call(
            functools.partial(kernel, cfg),
            out_shape=(
                jax.ShapeDtypeStruct((count, seq, width), BF16),
                jax.ShapeDtypeStruct((N_LATE, seq, width), BF16),
            ),
            in_specs=[anywhere] + [vmem] * 6 + [anywhere] * 6,
            out_specs=(anywhere, anywhere),
            scratch_shapes=[
                pltpu.VMEM((3, width, width), BF16),
                pltpu.VMEM((width, 3 * width), BF16),
                pltpu.VMEM((2, 3, heads, head_dim), BF16),
                pltpu.VMEM((1, 3 * width), F32),
                pltpu.VMEM((width, width), BF16),
                pltpu.VMEM((2, width, half_ff), BF16),
                pltpu.VMEM((2, 1, half_ff), BF16),
                pltpu.VMEM((2 * half_ff, width), BF16),
                pltpu.VMEM((relayed, width), BF16),
                pltpu.VMEM((relayed, width), BF16),
                pltpu.VMEM((IN_SLOTS, seq, width), BF16),
                pltpu.VMEM((OUT_SLOTS, seq, width), BF16),
                pltpu.VMEM((seq, width), BF16),
                pltpu.VMEM((seq, 3 * width), BF16),
                pltpu.VMEM((seq, width), BF16),
                pltpu.VMEM((seq, width), BF16),
                pltpu.VMEM((seq, 2 * half_ff), BF16),
                pltpu.SemaphoreType.DMA((9,)),
                pltpu.SemaphoreType.DMA((9,)),
                pltpu.SemaphoreType.DMA((9,)),
                pltpu.SemaphoreType.DMA((3,)),
                pltpu.SemaphoreType.DMA((2,)),
                pltpu.SemaphoreType.DMA((IN_SLOTS,)),
                pltpu.SemaphoreType.DMA((OUT_SLOTS,)),
                pltpu.SemaphoreType.DMA((OUT_SLOTS,)),
                pltpu.SemaphoreType.DMA((n_single,)),
                pltpu.SemaphoreType.DMA((n_single,)),
                pltpu.SemaphoreType.REGULAR,
                pltpu.SemaphoreType.REGULAR,
                pltpu.SemaphoreType.REGULAR,
            ],
            compiler_params=pltpu.CompilerParams(
                collective_id=0,
                has_side_effects=True,
                vmem_limit_bytes=60 * 2**20,
            ),
        )(*operands)
        late = lax.ppermute(late, "tp", [(0, 1), (1, 0)])
        out = pl.pallas_call(
            functools.partial(copy_kernel, n_single),
            out_shape=jax.ShapeDtypeStruct((count, seq, width), BF16),
            in_specs=[anywhere],
            out_specs=anywhere,
            scratch_shapes=[
                pltpu.VMEM((COPY_SLOTS, seq, width), BF16),
                pltpu.SemaphoreType.DMA((COPY_SLOTS,)),
                pltpu.SemaphoreType.DMA((COPY_SLOTS,)),
            ],
            compiler_params=pltpu.CompilerParams(vmem_limit_bytes=60 * 2**20),
            cost_estimate=pl.CostEstimate(
                flops=5 * 10**10, transcendentals=0, bytes_accessed=4 * count * seq * width
            ),
        )(out)
        first = (1 - lax.axis_index("tp")) * n_single + n_single - N_LATE
        out = lax.dynamic_update_slice(out, late, (first, 0, 0))
        return out.reshape(1, micro, rows, seq, width)

    return jax.shard_map(
        local_run,
        mesh=mesh,
        in_specs=(P(None, "dp", None, None),) + weight_specs,
        out_specs=P("pp", None, "dp", None, None),
        check_vma=False,
    )
```

```python
import functools
import math

import jax
import jax.numpy as jnp
from jax import lax
from jax.experimental import pallas as pl
from jax.experimental.pallas import tpu as pltpu
from jax.sharding import PartitionSpec as P

F32 = jnp.float32
BF16 = jnp.bfloat16
MESH = pl.DeviceIdType.MESH
LN_EPS = 1e-5
N_DUP = 18
N_LATE = 3
IN_SLOTS = 4
OUT_SLOTS = 8
HELD = 2
QUERY_BLOCK = 256
COL_BLOCK = 768
ROW_BLOCK = 128
MID_ROW_BLOCK = 256
COPY_SLOTS = 48
GELU_C0 = math.sqrt(2.0 / math.pi)
GELU_C1 = GELU_C0 * 0.044715


def dot(a, b, ca=1, cb=0):
    return lax.dot_general(a, b, (((ca,), (cb,)), ((), ())), preferred_element_type=F32)


def layer_norm(x, gain, bias):
    x = x.astype(F32)
    mean = jnp.mean(x, axis=-1, keepdims=True)
    centered = x - mean
    var = jnp.mean(centered * centered, axis=-1, keepdims=True)
    return (centered * lax.rsqrt(var + LN_EPS) * gain.astype(F32) + bias.astype(F32)).astype(BF16)


def gelu(z):
    return z * jax.nn.sigmoid(z * (2.0 * GELU_C0 + 2.0 * GELU_C1 * (z * z)))


def attention(qkv, ctx, head_dim):
    seq, width = ctx.shape
    pair = 2 * head_dim
    scale = head_dim**-0.5 * math.log2(math.e)
    first = lax.broadcasted_iota(jnp.int32, (1, pair), 1) < head_dim
    zero = jnp.zeros((), BF16)
    block = QUERY_BLOCK
    quarter = block // 2
    keep = lax.broadcasted_iota(jnp.int32, (quarter, quarter), 0) >= lax.broadcasted_iota(
        jnp.int32, (quarter, quarter), 1
    )
    hidden = jnp.full((quarter, quarter), -1e30, F32)
    for q0 in range(seq - block, -1, -block):
        for p in range(width // pair):
            lanes = slice(p * pair, (p + 1) * pair)
            keys = qkv[: q0 + block, width + p * pair : width + (p + 1) * pair]
            values = qkv[: q0 + block, 2 * width + p * pair : 2 * width + (p + 1) * pair]
            q = qkv[q0 : q0 + block, lanes]
            q = jnp.concatenate([jnp.where(first, q, zero), jnp.where(first, zero, q)], axis=0)
            scores = dot(q, keys, 1, 1)
            split, end = q0 + quarter, q0 + block
            rows = []
            for m in (0, block):
                upper = jnp.where(keep, scores[m : m + quarter, q0:split], -1e30)
                lower = jnp.where(keep, scores[m + quarter : m + block, split:end], -1e30)
                rows.append(jnp.concatenate([upper, hidden], axis=1))
                rows.append(jnp.concatenate([scores[m + quarter : m + block, q0:split], lower], axis=1))
            diag = jnp.concatenate(rows, axis=0)
            scores = jnp.concatenate([scores[:, :q0], diag], axis=1) if q0 else diag
            top = jnp.max(scores, axis=-1, keepdims=True)
            probs = jnp.exp2((scores - top) * scale)
            rows = []
            for m in (0, block):
                rows.append(jnp.concatenate([probs[m : m + quarter, :split], jnp.zeros_like(hidden)], axis=1))
                rows.append(probs[m + quarter : m + block])
            probs = jnp.concatenate(rows, axis=0)
            total = jnp.sum(probs, axis=-1, keepdims=True)
            out = dot(probs.astype(BF16), values) * (1.0 / total)
            ctx[q0 : q0 + block, lanes] = jnp.where(first, out[:block], out[block:]).astype(BF16)


def col_blocks(size):
    block = min(COL_BLOCK, size)
    return [slice(n, n + block) for n in range(0, size, block)]


def project_residual(lhs, weight, bias, resid, out, rows, cols):
    part = (dot(lhs[rows], weight[:, cols]) + bias[:, cols].astype(F32)).astype(BF16)
    out[rows, cols] = (resid[rows, cols].astype(F32) + part.astype(F32)).astype(BF16)


def one_layer(x, y, w, s, head_dim):
    seq, width = x.shape
    blocks = [slice(m, m + ROW_BLOCK) for m in range(0, seq, ROW_BLOCK)]
    for rows in blocks:
        s["h"][rows] = layer_norm(x[rows], w["g1"][...], w["c1"][...])
        for cols in col_blocks(3 * width):
            s["qkv"][rows, cols] = (dot(s["h"][rows], w["qkv"][:, cols]) + w["bqkv"][:, cols]).astype(BF16)
    attention(s["qkv"], s["ctx"], head_dim)
    for m in range(seq - MID_ROW_BLOCK, -1, -MID_ROW_BLOCK):
        rows = slice(m, m + MID_ROW_BLOCK)
        for cols in col_blocks(width):
            project_residual(s["ctx"], w["out"], w["bout"], x, s["x1"], rows, cols)
        s["h"][rows] = layer_norm(s["x1"][rows], w["g2"][...], w["c2"][...])
    half = w["up"].shape[2]
    blocks = blocks[len(blocks) // 2 :] + blocks[: len(blocks) // 2]
    for t in range(2):
        for cols in col_blocks(half):
            for rows in blocks:
                z = dot(s["h"][rows], w["up"][t, :, cols]) + w["bup"][t, :, cols].astype(F32)
                s["u"][rows, t * half + cols.start : t * half + cols.stop] = gelu(z).astype(BF16)
    for cols in col_blocks(width):
        for rows in blocks:
            project_residual(s["u"], w["down"], w["bdown"], s["x1"], y, rows, cols)


def kernel(
    cfg,
    x_hbm, g1, c1, bout, g2, c2, bdown, qkv_half, bqkv_half, out_half, up_half, bup_half, down_half,
    out_hbm, late_hbm,
    w_qkv_raw, w_qkv, b_qkv_raw, b_qkv, w_out, w_up, b_up, w_down,
    relay_a, relay_b, x_in, y_out, h, qkv, ctx, x1, u,
    w_local, w_send, w_recv, r_send, r_recv, in_sem, store_sem, hop_sem, side_send, side_recv, credit, turn, clear,
):
    stages, n_single, n_dup, head_dim = cfg
    n_early = n_single - late_hbm.shape[0]
    total = n_single + n_dup
    t = lax.axis_index("tp")
    p = lax.axis_index("pp")
    width = x_hbm.shape[2]
    half_width = width // 2
    other = {"tp": 1 - t}
    after = {"pp": lax.rem(p + 1, stages)}
    before = {"pp": lax.rem(p + stages - 1, stages)}

    across = {"pp": lax.rem(p + 2, stages)}

    barrier = pltpu.get_barrier_semaphore()
    for peer in (other, after, before, across):
        pl.semaphore_signal(barrier, inc=1, device_id=peer, device_id_type=MESH)
    pl.semaphore_wait(barrier, 4)

    half_ff = down_half.shape[0]
    mine = pl.ds(pl.multiple_of(t * half_width, 128), half_width)
    pieces = [(qkv_half.at[c], w_qkv_raw.at[c, mine]) for c in range(3)]
    pieces.append((bqkv_half, b_qkv_raw.at[t]))
    pieces.append((out_half, w_out.at[mine]))
    pieces.append((bup_half, b_up.at[t]))
    pieces.append((up_half, w_up.at[t]))
    relayed = relay_a.shape[0]
    direct = half_ff - relayed
    down_at = pl.multiple_of(t * half_ff, 128)
    pieces.append((down_half.at[:direct], w_down.at[pl.ds(down_at, direct)]))
    pieces.append((down_half.at[direct:], w_down.at[pl.ds(down_at + direct, relayed)]))
    near, far = [], []
    for i, (src, dst) in enumerate(pieces):
        near.append(pltpu.make_async_copy(src, dst, w_local.at[i]))
        far.append(
            pltpu.make_async_remote_copy(src, dst, w_send.at[i], w_recv.at[i], device_id=other, device_id_type=MESH)
        )
        near[-1].start()

    last = len(pieces) - 1
    far_down_at = pl.multiple_of((1 - t) * half_ff, 128)
    relay = [
        pltpu.make_async_remote_copy(src, dst, r_send.at[i], r_recv.at[i], device_id=to, device_id_type=MESH)
        for i, (src, dst, to) in enumerate(
            [(down_half.at[direct:], relay_a, across), (relay_a, relay_b, other)]
        )
    ]
    relay.append(
        pltpu.make_async_remote_copy(
            relay_b, w_down.at[pl.ds(far_down_at + direct, relayed)], r_send.at[2], w_recv.at[last],
            device_id=across, device_id_type=MESH,
        )
    )

    @pl.when(p == 1)
    def _():
        relay[0].start()

    @pl.when(p == 3)
    def _():
        relay[0].wait_recv()
        relay[1].start()
        relay[1].wait_recv()
        relay[2].start()

    @pl.when(lax.rem(p, 2) == 1)
    def _():
        pl.semaphore_wait(turn, 1)

    for copy in far[:last]:
        copy.start()

    @pl.when(p != 1)
    def _():
        far[last].start()

    mixed = n_early + n_dup

    share = -(-512 * n_dup // mixed)
    assert [m * share // 512 for m in (0, mixed)] == [0, n_dup]

    def dups_before(n):
        return lax.div(jnp.minimum(n, mixed) * share, 512)

    def single_index(n):
        return n - dups_before(n)

    def is_dup(n):
        return dups_before(n + 1) - dups_before(n)

    def row_of(n):
        dup = is_dup(n)
        return dup * (2 * n_single + dups_before(n)) + (1 - dup) * (t * n_single + single_index(n))

    def load(n):
        slot = lax.rem(n, IN_SLOTS)
        return pltpu.make_async_copy(x_hbm.at[row_of(n)], x_in.at[slot], in_sem.at[slot])

    def store(n):
        slot = lax.rem(n, OUT_SLOTS)
        return pltpu.make_async_copy(y_out.at[slot], out_hbm.at[row_of(n)], store_sem.at[slot])

    def hop(n):
        src, dst = lax.rem(n, OUT_SLOTS), lax.rem(n, IN_SLOTS)
        return pltpu.make_async_remote_copy(
            y_out.at[src], x_in.at[dst], hop_sem.at[src], in_sem.at[dst], device_id=after, device_id_type=MESH
        )

    def side(n):
        slot, k = lax.rem(n, OUT_SLOTS), single_index(n)
        return pltpu.make_async_remote_copy(
            y_out.at[slot], out_hbm.at[t * n_single + k], side_send.at[k], side_recv.at[k],
            device_id=other, device_id_type=MESH,
        )

    def keep_late(n):
        slot, k = lax.rem(n, OUT_SLOTS), single_index(n)
        return pltpu.make_async_copy(y_out.at[slot], late_hbm.at[k - n_early], side_send.at[k])

    def send_side(n):
        @pl.when((is_dup(n) == 0) & (single_index(n) < n_early))
        def _():
            side(n).start()

    def reuse(n):
        store(n).wait()

        @pl.when(p < stages - 1)
        def _():
            hop(n).wait_send()

        @pl.when((is_dup(n) == 0) & (single_index(n) < n_early))
        def _():
            side(n).wait_send()

        @pl.when((is_dup(n) == 0) & (single_index(n) >= n_early))
        def _():
            keep_late(n).wait()

    @pl.when(p == 0)
    def _():
        load(0).start()

    def arrived(i):
        near[i].wait()
        far[i].wait_recv()

    for i in range(4):
        arrived(i)
    for c in range(3):
        for m in range(0, width, QUERY_BLOCK):
            w_qkv[:, c * width + m : c * width + m + QUERY_BLOCK] = w_qkv_raw[c, m : m + QUERY_BLOCK, :].T
        for k in range(2):
            for head in range(half_width // head_dim):
                at = c * width + k * half_width + head * head_dim
                b_qkv[:, at : at + head_dim] = b_qkv_raw[k, c, head : head + 1, :].astype(F32)
    @pl.when(lax.rem(p, 2) == 0)
    def _():
        for copy in far[:7]:
            copy.wait_send()
        pl.semaphore_signal(turn, inc=1, device_id=after, device_id_type=MESH)

    for i in range(4, len(far)):
        arrived(i)

    @pl.when(p == 1)
    def _():
        for copy in far[:last]:
            copy.wait_send()
        pl.semaphore_signal(clear, inc=1, device_id=before, device_id_type=MESH)

    weights = dict(
        g1=g1, c1=c1, qkv=w_qkv, bqkv=b_qkv, out=w_out, bout=bout, g2=g2, c2=c2,
        up=w_up, bup=b_up, down=w_down, bdown=bdown,
    )
    scratch = dict(h=h, qkv=qkv, ctx=ctx, x1=x1, u=u)

    def step(n, carry):
        in_slot, out_slot = lax.rem(n, IN_SLOTS), lax.rem(n, OUT_SLOTS)
        load(n).wait()

        @pl.when((p == 0) & (n + 1 < total))
        def _():
            load(n + 1).start()

        @pl.when(n >= OUT_SLOTS)
        def _():
            reuse(n - OUT_SLOTS)

        single, k = is_dup(n) == 0, single_index(n)
        late = single & (k >= n_early)
        one_layer(x_in.at[in_slot], y_out.at[out_slot], weights, scratch, head_dim)

        @pl.when((p < stages - 1) & (n >= IN_SLOTS))
        def _():
            pl.semaphore_wait(credit, 1)

        @pl.when(p < stages - 1)
        def _():
            hop(n).start()

        @pl.when((p == 0) & (n == HELD))
        def _():
            pl.semaphore_wait(clear, 1)
            for m in range(HELD):
                send_side(m)

        @pl.when((p != 0) | (n >= HELD))
        def _():
            send_side(n)

        store(n).start()

        @pl.when(late)
        def _():
            keep_late(n).start()

        @pl.when((p > 0) & (n + IN_SLOTS < total))
        def _():
            pl.semaphore_signal(credit, inc=1, device_id=before, device_id_type=MESH)

        return carry

    lax.fori_loop(0, total, step, 0)
    def drain(n, carry):
        reuse(n)
        return carry

    lax.fori_loop(total - OUT_SLOTS, total, drain, 0)

    @pl.when(lax.rem(p, 2) == 0)
    def _():
        for copy in far[7:]:
            copy.wait_send()

    @pl.when(p == 3)
    def _():
        for copy in far:
            copy.wait_send()

    @pl.when(p == 1)
    def _():
        relay[0].wait_send()

    @pl.when(p == 3)
    def _():
        relay[1].wait_send()
        relay[2].wait_send()

    def finish(k, carry):
        row = (1 - t) * n_single + k
        pltpu.make_async_copy(out_hbm.at[row], out_hbm.at[row], side_recv.at[k]).wait()
        return carry

    lax.fori_loop(0, n_early, finish, 0)


def copy_kernel(n_single, src, dst, held, sem_in, sem_out):
    slots, count = held.shape[0], src.shape[0]
    begin = (1 - lax.axis_index("tp")) * n_single + n_single
    steps = count - N_LATE

    def row(i):
        return lax.rem(begin + i, count)

    def fetch(i):
        return pltpu.make_async_copy(src.at[row(i)], held.at[i % slots], sem_in.at[i % slots])

    def put(i):
        return pltpu.make_async_copy(held.at[i % slots], dst.at[row(i)], sem_out.at[i % slots])

    ahead = min(slots // 2, steps)
    for i in range(ahead):
        fetch(i).start()
    for i in range(steps):
        if i + ahead < steps:
            if i + ahead >= slots:
                put(i + ahead - slots).wait()
            fetch(i + ahead).start()
        fetch(i).wait()
        put(i).start()
    for i in range(max(steps - slots, 0), steps):
        put(i).wait()


def solution(mesh):
    stages = mesh.shape["pp"]
    weight_specs = (
        P("pp", None), P("pp", None),
        P("pp", None, None, "tp", None), P("pp", None, "tp", None),
        P("pp", "tp", None, None), P("pp", None),
        P("pp", None), P("pp", None),
        P("pp", None, "tp"), P("pp", "tp"),
        P("pp", "tp", None), P("pp", None),
    )

    def local_run(x_micro, g1, c1, w_qkv, b_qkv, w_out, b_out, g2, c2, w_up, b_up, w_down, b_down):
        micro, rows, seq, width = x_micro.shape
        count = micro * rows
        heads, head_dim = w_qkv.shape[3:]
        half_width = heads * head_dim
        half_ff = w_up.shape[2]
        relayed = 2 * half_ff // 3 // 128 * 128
        n_dup = N_DUP
        n_single = (count - n_dup) // 2
        cfg = (stages, n_single, n_dup, head_dim)
        operands = (
            x_micro.reshape(count, seq, width),
            g1, c1, b_out, g2, c2, b_down,
            w_qkv.reshape(3, width, heads, head_dim).transpose(0, 2, 3, 1).reshape(3, half_width, width),
            b_qkv.reshape(3, heads, head_dim),
            w_out.reshape(half_width, width),
            w_up.reshape(width, half_ff),
            b_up.reshape(1, half_ff),
            w_down.reshape(half_ff, width),
        )
        anywhere = pl.BlockSpec(memory_space=pl.ANY)
        vmem = pl.BlockSpec(memory_space=pltpu.VMEM)
        out, late = pl.pallas_call(
            functools.partial(kernel, cfg),
            out_shape=(
                jax.ShapeDtypeStruct((count, seq, width), BF16),
                jax.ShapeDtypeStruct((N_LATE, seq, width), BF16),
            ),
            in_specs=[anywhere] + [vmem] * 6 + [anywhere] * 6,
            out_specs=(anywhere, anywhere),
            scratch_shapes=[
                pltpu.VMEM((3, width, width), BF16),
                pltpu.VMEM((width, 3 * width), BF16),
                pltpu.VMEM((2, 3, heads, head_dim), BF16),
                pltpu.VMEM((1, 3 * width), F32),
                pltpu.VMEM((width, width), BF16),
                pltpu.VMEM((2, width, half_ff), BF16),
                pltpu.VMEM((2, 1, half_ff), BF16),
                pltpu.VMEM((2 * half_ff, width), BF16),
                pltpu.VMEM((relayed, width), BF16),
                pltpu.VMEM((relayed, width), BF16),
                pltpu.VMEM((IN_SLOTS, seq, width), BF16),
                pltpu.VMEM((OUT_SLOTS, seq, width), BF16),
                pltpu.VMEM((seq, width), BF16),
                pltpu.VMEM((seq, 3 * width), BF16),
                pltpu.VMEM((seq, width), BF16),
                pltpu.VMEM((seq, width), BF16),
                pltpu.VMEM((seq, 2 * half_ff), BF16),
                pltpu.SemaphoreType.DMA((9,)),
                pltpu.SemaphoreType.DMA((9,)),
                pltpu.SemaphoreType.DMA((9,)),
                pltpu.SemaphoreType.DMA((3,)),
                pltpu.SemaphoreType.DMA((2,)),
                pltpu.SemaphoreType.DMA((IN_SLOTS,)),
                pltpu.SemaphoreType.DMA((OUT_SLOTS,)),
                pltpu.SemaphoreType.DMA((OUT_SLOTS,)),
                pltpu.SemaphoreType.DMA((n_single,)),
                pltpu.SemaphoreType.DMA((n_single,)),
                pltpu.SemaphoreType.REGULAR,
                pltpu.SemaphoreType.REGULAR,
                pltpu.SemaphoreType.REGULAR,
            ],
            compiler_params=pltpu.CompilerParams(
                collective_id=0,
                has_side_effects=True,
                vmem_limit_bytes=60 * 2**20,
            ),
        )(*operands)
        late = lax.ppermute(late, "tp", [(0, 1), (1, 0)])
        out = pl.pallas_call(
            functools.partial(copy_kernel, n_single),
            out_shape=jax.ShapeDtypeStruct((count, seq, width), BF16),
            in_specs=[anywhere],
            out_specs=anywhere,
            scratch_shapes=[
                pltpu.VMEM((COPY_SLOTS, seq, width), BF16),
                pltpu.SemaphoreType.DMA((COPY_SLOTS,)),
                pltpu.SemaphoreType.DMA((COPY_SLOTS,)),
            ],
            compiler_params=pltpu.CompilerParams(vmem_limit_bytes=60 * 2**20),
            cost_estimate=pl.CostEstimate(
                flops=5 * 10**10, transcendentals=0, bytes_accessed=4 * count * seq * width
            ),
        )(out)
        first = (1 - lax.axis_index("tp")) * n_single + n_single - N_LATE
        out = lax.dynamic_update_slice(out, late, (first, 0, 0))
        return out.reshape(1, micro, rows, seq, width)

    return jax.shard_map(
        local_run,
        mesh=mesh,
        in_specs=(P(None, "dp", None, None),) + weight_specs,
        out_specs=P("pp", None, "dp", None, None),
        check_vma=False,
    )
```

```python
import functools
import math

import jax
import jax.numpy as jnp
from jax import lax
from jax.experimental import pallas as pl
from jax.experimental.pallas import tpu as pltpu
from jax.sharding import PartitionSpec as P

F32 = jnp.float32
BF16 = jnp.bfloat16
MESH = pl.DeviceIdType.MESH
LN_EPS = 1e-5
N_DUP = 18
N_LATE = 3
IN_SLOTS = 4
OUT_SLOTS = 8
HELD = 2
QUERY_BLOCK = 256
COL_BLOCK = 768
ROW_BLOCK = 128
MID_ROW_BLOCK = 256
COPY_SLOTS = 48
GELU_C0 = math.sqrt(2.0 / math.pi)
GELU_C1 = GELU_C0 * 0.044715


def dot(a, b, ca=1, cb=0):
    return lax.dot_general(a, b, (((ca,), (cb,)), ((), ())), preferred_element_type=F32)


def layer_norm(x, gain, bias):
    x = x.astype(F32)
    mean = jnp.mean(x, axis=-1, keepdims=True)
    centered = x - mean
    var = jnp.mean(centered * centered, axis=-1, keepdims=True)
    return (centered * lax.rsqrt(var + LN_EPS) * gain.astype(F32) + bias.astype(F32)).astype(BF16)


def gelu(z):
    return z * jax.nn.sigmoid(z * (2.0 * GELU_C0 + 2.0 * GELU_C1 * (z * z)))


def attention(qkv, ctx, head_dim):
    seq, width = ctx.shape
    pair = 2 * head_dim
    scale = head_dim**-0.5 * math.log2(math.e)
    first = lax.broadcasted_iota(jnp.int32, (1, pair), 1) < head_dim
    zero = jnp.zeros((), BF16)
    block = QUERY_BLOCK
    quarter = block // 2
    keep = lax.broadcasted_iota(jnp.int32, (quarter, quarter), 0) >= lax.broadcasted_iota(
        jnp.int32, (quarter, quarter), 1
    )
    hidden = jnp.full((quarter, quarter), -1e30, F32)
    for q0 in range(seq - block, -1, -block):
        for p in range(width // pair):
            lanes = slice(p * pair, (p + 1) * pair)
            keys = qkv[: q0 + block, width + p * pair : width + (p + 1) * pair]
            values = qkv[: q0 + block, 2 * width + p * pair : 2 * width + (p + 1) * pair]
            q = qkv[q0 : q0 + block, lanes]
            q = jnp.concatenate([jnp.where(first, q, zero), jnp.where(first, zero, q)], axis=0)
            scores = dot(q, keys, 1, 1)
            split, end = q0 + quarter, q0 + block
            rows = []
            for m in (0, block):
                upper = jnp.where(keep, scores[m : m + quarter, q0:split], -1e30)
                lower = jnp.where(keep, scores[m + quarter : m + block, split:end], -1e30)
                rows.append(jnp.concatenate([upper, hidden], axis=1))
                rows.append(jnp.concatenate([scores[m + quarter : m + block, q0:split], lower], axis=1))
            diag = jnp.concatenate(rows, axis=0)
            scores = jnp.concatenate([scores[:, :q0], diag], axis=1) if q0 else diag
            top = jnp.max(scores, axis=-1, keepdims=True)
            probs = jnp.exp2((scores - top) * scale)
            rows = []
            for m in (0, block):
                rows.append(jnp.concatenate([probs[m : m + quarter, :split], jnp.zeros_like(hidden)], axis=1))
                rows.append(probs[m + quarter : m + block])
            probs = jnp.concatenate(rows, axis=0)
            total = jnp.sum(probs, axis=-1, keepdims=True)
            out = dot(probs.astype(BF16), values) * (1.0 / total)
            ctx[q0 : q0 + block, lanes] = jnp.where(first, out[:block], out[block:]).astype(BF16)


def col_blocks(size, most=COL_BLOCK):
    block = min(most, size)
    return [slice(n, n + block) for n in range(0, size, block)]


def project_residual(lhs, weight, bias, resid, out, rows, cols):
    part = (dot(lhs[rows], weight[:, cols]) + bias[:, cols].astype(F32)).astype(BF16)
    out[rows, cols] = (resid[rows, cols].astype(F32) + part.astype(F32)).astype(BF16)


def one_layer(x, y, w, s, head_dim):
    seq, width = x.shape
    blocks = [slice(m, m + ROW_BLOCK) for m in range(0, seq, ROW_BLOCK)]
    for rows in blocks:
        s["h"][rows] = layer_norm(x[rows], w["g1"][...], w["c1"][...])
        for cols in col_blocks(3 * width):
            s["qkv"][rows, cols] = (dot(s["h"][rows], w["qkv"][:, cols]) + w["bqkv"][:, cols]).astype(BF16)
    attention(s["qkv"], s["ctx"], head_dim)
    for m in range(seq - MID_ROW_BLOCK, -1, -MID_ROW_BLOCK):
        rows = slice(m, m + MID_ROW_BLOCK)
        for cols in col_blocks(width):
            project_residual(s["ctx"], w["out"], w["bout"], x, s["x1"], rows, cols)
        s["h"][rows] = layer_norm(s["x1"][rows], w["g2"][...], w["c2"][...])
    half = w["up"].shape[2]
    blocks = blocks[len(blocks) // 2 :] + blocks[: len(blocks) // 2]
    for t in range(2):
        for cols in col_blocks(half, 2 * COL_BLOCK):
            for rows in blocks:
                z = dot(s["h"][rows], w["up"][t, :, cols]) + w["bup"][t, :, cols].astype(F32)
                s["u"][rows, t * half + cols.start : t * half + cols.stop] = gelu(z).astype(BF16)
    for cols in col_blocks(width):
        for m in range(seq - MID_ROW_BLOCK, -1, -MID_ROW_BLOCK):
            rows = slice(m, m + MID_ROW_BLOCK)
            project_residual(s["u"], w["down"], w["bdown"], s["x1"], y, rows, cols)


def kernel(
    cfg,
    x_hbm, g1, c1, bout, g2, c2, bdown, qkv_half, bqkv_half, out_half, up_half, bup_half, down_half,
    out_hbm, late_hbm,
    w_qkv_raw, w_qkv, b_qkv_raw, b_qkv, w_out, w_up, b_up, w_down,
    relay_a, relay_b, x_in, y_out, h, qkv, ctx, x1, u,
    w_local, w_send, w_recv, r_send, r_recv, in_sem, store_sem, hop_sem, side_send, side_recv, credit, turn, clear,
):
    stages, n_single, n_dup, head_dim = cfg
    n_early = n_single - late_hbm.shape[0]
    total = n_single + n_dup
    t = lax.axis_index("tp")
    p = lax.axis_index("pp")
    width = x_hbm.shape[2]
    half_width = width // 2
    other = {"tp": 1 - t}
    after = {"pp": lax.rem(p + 1, stages)}
    before = {"pp": lax.rem(p + stages - 1, stages)}

    across = {"pp": lax.rem(p + 2, stages)}

    barrier = pltpu.get_barrier_semaphore()
    for peer in (other, after, before, across):
        pl.semaphore_signal(barrier, inc=1, device_id=peer, device_id_type=MESH)
    pl.semaphore_wait(barrier, 4)

    half_ff = down_half.shape[0]
    mine = pl.ds(pl.multiple_of(t * half_width, 128), half_width)
    pieces = [(qkv_half.at[c], w_qkv_raw.at[c, mine]) for c in range(3)]
    pieces.append((bqkv_half, b_qkv_raw.at[t]))
    pieces.append((out_half, w_out.at[mine]))
    pieces.append((bup_half, b_up.at[t]))
    pieces.append((up_half, w_up.at[t]))
    relayed = relay_a.shape[0]
    direct = half_ff - relayed
    down_at = pl.multiple_of(t * half_ff, 128)
    pieces.append((down_half.at[:direct], w_down.at[pl.ds(down_at, direct)]))
    pieces.append((down_half.at[direct:], w_down.at[pl.ds(down_at + direct, relayed)]))
    near, far = [], []
    for i, (src, dst) in enumerate(pieces):
        near.append(pltpu.make_async_copy(src, dst, w_local.at[i]))
        far.append(
            pltpu.make_async_remote_copy(src, dst, w_send.at[i], w_recv.at[i], device_id=other, device_id_type=MESH)
        )
        near[-1].start()

    last = len(pieces) - 1
    far_down_at = pl.multiple_of((1 - t) * half_ff, 128)
    relay = [
        pltpu.make_async_remote_copy(src, dst, r_send.at[i], r_recv.at[i], device_id=to, device_id_type=MESH)
        for i, (src, dst, to) in enumerate(
            [(down_half.at[direct:], relay_a, across), (relay_a, relay_b, other)]
        )
    ]
    relay.append(
        pltpu.make_async_remote_copy(
            relay_b, w_down.at[pl.ds(far_down_at + direct, relayed)], r_send.at[2], w_recv.at[last],
            device_id=across, device_id_type=MESH,
        )
    )

    @pl.when(p == 1)
    def _():
        relay[0].start()

    @pl.when(p == 3)
    def _():
        relay[0].wait_recv()
        relay[1].start()
        relay[1].wait_recv()
        relay[2].start()

    @pl.when(lax.rem(p, 2) == 1)
    def _():
        pl.semaphore_wait(turn, 1)

    for copy in far[:last]:
        copy.start()

    @pl.when(p != 1)
    def _():
        far[last].start()

    mixed = n_early + n_dup

    share = -(-512 * n_dup // mixed)
    assert [m * share // 512 for m in (0, mixed)] == [0, n_dup]

    def dups_before(n):
        return lax.div(jnp.minimum(n, mixed) * share, 512)

    def single_index(n):
        return n - dups_before(n)

    def is_dup(n):
        return dups_before(n + 1) - dups_before(n)

    def row_of(n):
        dup = is_dup(n)
        return dup * (2 * n_single + dups_before(n)) + (1 - dup) * (t * n_single + single_index(n))

    def load(n, row=0):
        slot = lax.rem(n, IN_SLOTS)
        return pltpu.make_async_copy(x_hbm.at[row], x_in.at[slot], in_sem.at[slot])

    def store(n, row=0):
        slot = lax.rem(n, OUT_SLOTS)
        return pltpu.make_async_copy(y_out.at[slot], out_hbm.at[row], store_sem.at[slot])

    def hop(n):
        src, dst = lax.rem(n, OUT_SLOTS), lax.rem(n, IN_SLOTS)
        return pltpu.make_async_remote_copy(
            y_out.at[src], x_in.at[dst], hop_sem.at[src], in_sem.at[dst], device_id=after, device_id_type=MESH
        )

    def side(n, k):
        return pltpu.make_async_remote_copy(
            y_out.at[lax.rem(n, OUT_SLOTS)], out_hbm.at[t * n_single + k], side_send.at[k], side_recv.at[k],
            device_id=other, device_id_type=MESH,
        )

    def keep_late(n, k):
        return pltpu.make_async_copy(y_out.at[lax.rem(n, OUT_SLOTS)], late_hbm.at[k - n_early], side_send.at[k])

    def kind(n):
        single, k = is_dup(n) == 0, single_index(n)
        return single & (k < n_early), single & (k >= n_early), k

    def reuse(n, early, late, k):
        store(n).wait()

        @pl.when(p < stages - 1)
        def _():
            hop(n).wait_send()

        @pl.when(early)
        def _():
            side(n, k).wait_send()

        @pl.when(late)
        def _():
            keep_late(n, k).wait()

    @pl.when(p == 0)
    def _():
        load(0, row_of(0)).start()
        load(1, row_of(1)).start()

    def arrived(i):
        near[i].wait()
        far[i].wait_recv()

    for i in range(4):
        arrived(i)
    for c in range(3):
        for m in range(0, width, QUERY_BLOCK):
            w_qkv[:, c * width + m : c * width + m + QUERY_BLOCK] = w_qkv_raw[c, m : m + QUERY_BLOCK, :].T
        for k in range(2):
            for head in range(half_width // head_dim):
                at = c * width + k * half_width + head * head_dim
                b_qkv[:, at : at + head_dim] = b_qkv_raw[k, c, head : head + 1, :].astype(F32)
    @pl.when(lax.rem(p, 2) == 0)
    def _():
        for copy in far[:7]:
            copy.wait_send()
        pl.semaphore_signal(turn, inc=1, device_id=after, device_id_type=MESH)

    for i in range(4, len(far)):
        arrived(i)

    @pl.when(p == 1)
    def _():
        for copy in far[:last]:
            copy.wait_send()
        pl.semaphore_signal(clear, inc=1, device_id=before, device_id_type=MESH)

    weights = dict(
        g1=g1, c1=c1, qkv=w_qkv, bqkv=b_qkv, out=w_out, bout=bout, g2=g2, c2=c2,
        up=w_up, bup=b_up, down=w_down, bdown=bdown,
    )
    scratch = dict(h=h, qkv=qkv, ctx=ctx, x1=x1, u=u)

    def step(n, carry):
        in_slot, out_slot = lax.rem(n, IN_SLOTS), lax.rem(n, OUT_SLOTS)
        load(n).wait()

        row = row_of(n)
        early, late, k = kind(n)
        old = n + 1 - OUT_SLOTS
        old_kind = kind(old)
        ahead_row = row_of(n + 2)
        one_layer(x_in.at[in_slot], y_out.at[out_slot], weights, scratch, head_dim)

        @pl.when((p < stages - 1) & (n >= IN_SLOTS))
        def _():
            pl.semaphore_wait(credit, 1)

        @pl.when(p < stages - 1)
        def _():
            hop(n).start()

        @pl.when((p == 0) & (n == HELD))
        def _():
            pl.semaphore_wait(clear, 1)
            for m in range(HELD):
                m_early, _, m_k = kind(m)

                @pl.when(m_early)
                def _():
                    side(m, m_k).start()

        @pl.when(early & ((p != 0) | (n >= HELD)))
        def _():
            side(n, k).start()

        store(n, row).start()

        @pl.when(late)
        def _():
            keep_late(n, k).start()

        @pl.when((p > 0) & (n + IN_SLOTS < total))
        def _():
            pl.semaphore_signal(credit, inc=1, device_id=before, device_id_type=MESH)

        @pl.when((p == 0) & (n + 2 < total))
        def _():
            load(n + 2, ahead_row).start()

        @pl.when((old >= 0) & (n + 1 < total))
        def _():
            reuse(old, *old_kind)

        return carry

    lax.fori_loop(0, total, step, 0)

    def drain(n, carry):
        reuse(n, *kind(n))
        return carry

    lax.fori_loop(total - OUT_SLOTS, total, drain, 0)

    @pl.when(lax.rem(p, 2) == 0)
    def _():
        for copy in far[7:]:
            copy.wait_send()

    @pl.when(p == 3)
    def _():
        for copy in far:
            copy.wait_send()

    @pl.when(p == 1)
    def _():
        relay[0].wait_send()

    @pl.when(p == 3)
    def _():
        relay[1].wait_send()
        relay[2].wait_send()

    def finish(k, carry):
        row = (1 - t) * n_single + k
        pltpu.make_async_copy(out_hbm.at[row], out_hbm.at[row], side_recv.at[k]).wait()
        return carry

    lax.fori_loop(0, n_early, finish, 0)


def copy_kernel(n_single, src, dst, held, sem_in, sem_out):
    slots, count = held.shape[0], src.shape[0]
    begin = (1 - lax.axis_index("tp")) * n_single + n_single
    steps = count - N_LATE

    def row(i):
        return lax.rem(begin + i, count)

    def fetch(i):
        return pltpu.make_async_copy(src.at[row(i)], held.at[i % slots], sem_in.at[i % slots])

    def put(i):
        return pltpu.make_async_copy(held.at[i % slots], dst.at[row(i)], sem_out.at[i % slots])

    ahead = min(slots // 2, steps)
    for i in range(ahead):
        fetch(i).start()
    for i in range(steps):
        if i + ahead < steps:
            if i + ahead >= slots:
                put(i + ahead - slots).wait()
            fetch(i + ahead).start()
        fetch(i).wait()
        put(i).start()
    for i in range(max(steps - slots, 0), steps):
        put(i).wait()


def solution(mesh):
    stages = mesh.shape["pp"]
    weight_specs = (
        P("pp", None), P("pp", None),
        P("pp", None, None, "tp", None), P("pp", None, "tp", None),
        P("pp", "tp", None, None), P("pp", None),
        P("pp", None), P("pp", None),
        P("pp", None, "tp"), P("pp", "tp"),
        P("pp", "tp", None), P("pp", None),
    )

    def local_run(x_micro, g1, c1, w_qkv, b_qkv, w_out, b_out, g2, c2, w_up, b_up, w_down, b_down):
        micro, rows, seq, width = x_micro.shape
        count = micro * rows
        heads, head_dim = w_qkv.shape[3:]
        half_width = heads * head_dim
        half_ff = w_up.shape[2]
        relayed = 2 * half_ff // 3 // 128 * 128
        n_dup = N_DUP
        n_single = (count - n_dup) // 2
        cfg = (stages, n_single, n_dup, head_dim)
        operands = (
            x_micro.reshape(count, seq, width),
            g1, c1, b_out, g2, c2, b_down,
            w_qkv.reshape(3, width, heads, head_dim).transpose(0, 2, 3, 1).reshape(3, half_width, width),
            b_qkv.reshape(3, heads, head_dim),
            w_out.reshape(half_width, width),
            w_up.reshape(width, half_ff),
            b_up.reshape(1, half_ff),
            w_down.reshape(half_ff, width),
        )
        anywhere = pl.BlockSpec(memory_space=pl.ANY)
        vmem = pl.BlockSpec(memory_space=pltpu.VMEM)
        out, late = pl.pallas_call(
            functools.partial(kernel, cfg),
            out_shape=(
                jax.ShapeDtypeStruct((count, seq, width), BF16),
                jax.ShapeDtypeStruct((N_LATE, seq, width), BF16),
            ),
            in_specs=[anywhere] + [vmem] * 6 + [anywhere] * 6,
            out_specs=(anywhere, anywhere),
            scratch_shapes=[
                pltpu.VMEM((3, width, width), BF16),
                pltpu.VMEM((width, 3 * width), BF16),
                pltpu.VMEM((2, 3, heads, head_dim), BF16),
                pltpu.VMEM((1, 3 * width), F32),
                pltpu.VMEM((width, width), BF16),
                pltpu.VMEM((2, width, half_ff), BF16),
                pltpu.VMEM((2, 1, half_ff), BF16),
                pltpu.VMEM((2 * half_ff, width), BF16),
                pltpu.VMEM((relayed, width), BF16),
                pltpu.VMEM((relayed, width), BF16),
                pltpu.VMEM((IN_SLOTS, seq, width), BF16),
                pltpu.VMEM((OUT_SLOTS, seq, width), BF16),
                pltpu.VMEM((seq, width), BF16),
                pltpu.VMEM((seq, 3 * width), BF16),
                pltpu.VMEM((seq, width), BF16),
                pltpu.VMEM((seq, width), BF16),
                pltpu.VMEM((seq, 2 * half_ff), BF16),
                pltpu.SemaphoreType.DMA((9,)),
                pltpu.SemaphoreType.DMA((9,)),
                pltpu.SemaphoreType.DMA((9,)),
                pltpu.SemaphoreType.DMA((3,)),
                pltpu.SemaphoreType.DMA((2,)),
                pltpu.SemaphoreType.DMA((IN_SLOTS,)),
                pltpu.SemaphoreType.DMA((OUT_SLOTS,)),
                pltpu.SemaphoreType.DMA((OUT_SLOTS,)),
                pltpu.SemaphoreType.DMA((n_single,)),
                pltpu.SemaphoreType.DMA((n_single,)),
                pltpu.SemaphoreType.REGULAR,
                pltpu.SemaphoreType.REGULAR,
                pltpu.SemaphoreType.REGULAR,
            ],
            compiler_params=pltpu.CompilerParams(
                collective_id=0,
                has_side_effects=True,
                vmem_limit_bytes=60 * 2**20,
            ),
        )(*operands)
        late = lax.ppermute(late, "tp", [(0, 1), (1, 0)])
        out = pl.pallas_call(
            functools.partial(copy_kernel, n_single),
            out_shape=jax.ShapeDtypeStruct((count, seq, width), BF16),
            in_specs=[anywhere],
            out_specs=anywhere,
            scratch_shapes=[
                pltpu.VMEM((COPY_SLOTS, seq, width), BF16),
                pltpu.SemaphoreType.DMA((COPY_SLOTS,)),
                pltpu.SemaphoreType.DMA((COPY_SLOTS,)),
            ],
            compiler_params=pltpu.CompilerParams(vmem_limit_bytes=60 * 2**20),
            cost_estimate=pl.CostEstimate(
                flops=5 * 10**10, transcendentals=0, bytes_accessed=4 * count * seq * width
            ),
        )(out)
        first = (1 - lax.axis_index("tp")) * n_single + n_single - N_LATE
        out = lax.dynamic_update_slice(out, late, (first, 0, 0))
        return out.reshape(1, micro, rows, seq, width)

    return jax.shard_map(
        local_run,
        mesh=mesh,
        in_specs=(P(None, "dp", None, None),) + weight_specs,
        out_specs=P("pp", None, "dp", None, None),
        check_vma=False,
    )
```
